512 devices in a mesh: fluid: 32 (over y, x), solid: 16 (over z, core).
Axes of the slice: x: 4, y: 8, z: 8, core: 2. Of those that a mesh axis runs over, the one named last changes fastest.
Arguments:
- earlier_thermal_state: float32 [1024, 512, 128], P('fluid', 'solid'), may hold values from -6 to 6
- thermal_inertia: float32 [1024, 512, 128], P('fluid', 'solid'), may hold values from 0.3 to 3
- boundary_energy_current: float32 [64, 262144], P(None, ('fluid', 'solid')), may hold values from -6 to 6
- jacobian_quad_factors: float32 [64, 524288], P(None, ('fluid', 'solid')), may hold values from 0.05 to 0.4
- patch_holder_liquid: int32 [524288, 1], P(('fluid', 'solid')), may hold values from 0 to 31; in each aligned block of 1024 rows (0 to 1023, 1024 to 2047, ...) at most 128 rows name the same one
- patch_slot_number: int32 [524288], P(('fluid', 'solid')), may hold values from 0 to 511
Outputs:
- thermal_state_guess: float32 [1024, 512, 128], P('fluid', 'solid')
- equation_misfit: float32 [1024, 512, 128], P('fluid', 'solid')
The draws below stay inside these ranges and needn't reach their ends.
Inputs may be any that keep to these rules, and one draw needn't show every extreme that they name: `patch_holder_liquid`: within the rows of one device, no owner index is named by more than 128 rows; in the rows of some device one owner index is named by exactly 128 rows.
All inputs are finite; a program needn't handle non-finite values.
Results may differ from the reference program's by a relative error of at most 0.00025.
Values sent between devices are 32-bit elements; how exact they have to be, the bound alone decides.
A program may use at most 64 MiB of HBM per device.

```python
import math
import jax
import jax.numpy as jnp
import numpy as np

CX = 32
CY = 32
FACE_DEV = 512
Q = 64
ITERS = 3
ICELLS = 1024
MOST = 128
SOLID_COUNT_X = 1024
SOLID_COUNT_Y = 512
SOLID_COUNT_Z = 128
ROWS = 524288
FACES = 262144
N_FLUID = 32
N_SOLID = 16


def touch_ends(drawn, rng, smallest, high):
    spot = [jax.random.randint(jax.random.fold_in(rng, axis), (), 0, length) for axis, length in enumerate(drawn.shape)]
    main_axis = drawn.shape.index(max(drawn.shape))
    next_to = spot[:main_axis] + [(spot[main_axis] + 1) % drawn.shape[main_axis]] + spot[main_axis + 1:]
    return drawn.at[tuple(spot)].set(smallest).at[tuple(next_to)].set(high)


def level_of(own_key, shape, cuts, low, top_value):
    def one(axis_at, parts):
        heights = jax.random.uniform(jax.random.fold_in(jax.random.fold_in(own_key, 6), axis_at), (parts,), jnp.float32, low / len(cuts), top_value / len(cuts))
        return jnp.repeat(jnp.exp(heights), shape[axis_at] // parts).reshape((-1,) + (1,) * (len(shape) - axis_at - 1))

    factor_of = one(*cuts[0])
    for cut in cuts[1:]:
        factor_of = factor_of * one(*cut)
    return factor_of


def assign_block(own_key, own, number, rows, count, top, reach, lean):
    order = jax.random.permutation(own_key, count)
    packed, usual = portions_of(count, rows * top, reach, lean, True), portions_of(count, rows * top, reach, lean, False)
    places = jnp.arange(count)

    def named(sizes, turn):
        used = int((sizes > 0).sum())
        fixed = max(1, used // 4)
        passed = fixed + (places - fixed + turn * (used - fixed)) % max(1, count - fixed)
        return jnp.zeros((count,), jnp.int32).at[order[jnp.where(places < fixed, places, passed)]].set(jnp.asarray(sizes, jnp.int32))

    sizes = jnp.where(number % 4 == 0, named(packed, number // 4), named(usual, number - number // 4 - 1))
    mixed = jax.random.permutation(jax.random.fold_in(own, 3), count)
    donor, receiver = mixed[0:count // 2 * 2:2], mixed[1:count // 2 * 2:2]
    margin = jnp.minimum(sizes[donor] - 1, reach - sizes[receiver]) // 2
    margin = jnp.where((donor == order[0]) | (receiver == order[0]) | (sizes[receiver] == 0), 0, jnp.maximum(margin, 0))
    passed = jax.random.randint(jax.random.fold_in(own, 4), (count // 2,), 0, 1 << 20) % (margin + 1)
    sizes = sizes.at[donor].add(-passed).at[receiver].add(passed)
    items = jnp.searchsorted(jnp.cumsum(sizes), jnp.arange(rows * top), side="right").astype(jnp.int32)
    grid = items.reshape(top, rows).T
    grid = grid[jax.random.permutation(jax.random.fold_in(own, 1), rows)]
    turn = jax.random.randint(jax.random.fold_in(own, 2), (rows, 1), 0, top)
    return jnp.take_along_axis(grid, (jnp.arange(top)[None, :] + turn) % top, axis=1)


def portions_of(amount, total, bound, slope, full):
    weights = [(1 << 20) // math.isqrt(standing ** slope) + 1 for standing in range(1, amount + 1)]
    largest = bound if full else min(bound, max(-(-total // amount), total * weights[0] // sum(weights)))
    least = 1 if total - largest >= amount - 1 else 0
    given, rest = [largest] + [least] * (amount - 1), total - largest - least * (amount - 1)
    while rest > 0:
        free = [i for i in range(1, amount) if given[i] < largest] or [i for i in range(1, amount) if given[i] < bound]
        pool, left = sum([weights[i] for i in free]), rest
        for i in free:
            more = min(bound - given[i], max(1, left * weights[i] // pool), rest)
            given[i] = given[i] + more
            rest = rest - more
    return np.array(given)


def scatter_about(own_key, shape, spread, reach, cuts=(), kind=jnp.bfloat16):
    result = jax.random.normal(own_key, shape, jnp.float32) * spread
    if len(cuts) > 0:
        result = level_of(own_key, shape, cuts, -0.22, 0.18) * result
    return jnp.clip(result, min=-reach, max=reach).astype(kind)


def setup_inputs(seed: int = 0) -> dict:
    key_list = jax.random.split(jax.random.key(seed), 7)
    earlier_thermal_state = scatter_about(key_list[0], (SOLID_COUNT_X, SOLID_COUNT_Y, SOLID_COUNT_Z), 1.0, 6.0, ((0, 32), (1, 16)), jnp.float32)
    thermal_inertia = jnp.clip(jnp.exp(math.log(3.0) - 2.3025851 * jax.random.uniform(key_list[1], (SOLID_COUNT_X, SOLID_COUNT_Y, SOLID_COUNT_Z), jnp.float32) ** level_of(key_list[1], (SOLID_COUNT_X, SOLID_COUNT_Y, SOLID_COUNT_Z), ((0, 32), (1, 16)), -0.2, 0.2)), 0.3, 3.0)
    boundary_energy_current = scatter_about(key_list[2], (Q, FACES), 1.0, 6.0, ((1, 512),), jnp.float32)
    jacobian_quad_factors = jnp.clip(jnp.exp(math.log(0.4) - 2.0794415 * jax.random.uniform(key_list[3], (Q, ROWS), jnp.float32) ** level_of(key_list[3], (Q, ROWS), ((1, 512),), -0.2, 0.2)), 0.05, 0.4)
    patch_holder_liquid_keys = jax.random.split(jax.random.fold_in(key_list[4], 1), ROWS // ICELLS)
    patch_holder_liquid_turns = jax.random.permutation(jax.random.fold_in(key_list[4], 3), ROWS // ICELLS)
    patch_holder_liquid = jax.vmap(lambda own, number: assign_block(jax.random.fold_in(key_list[4], 2), own, number, ICELLS, N_FLUID, 1, MOST, 2))(patch_holder_liquid_keys, patch_holder_liquid_turns).reshape((ROWS, 1))
    patch_slot_number = touch_ends(jax.random.randint(key_list[5], (ROWS,), 0, FACE_DEV), jax.random.fold_in(key_list[5], 1), 0, FACE_DEV - 1).astype(jnp.int32)
    return {"earlier_thermal_state": earlier_thermal_state, "thermal_inertia": thermal_inertia, "boundary_energy_current": boundary_energy_current, "jacobian_quad_factors": jacobian_quad_factors, "patch_holder_liquid": patch_holder_liquid, "patch_slot_number": patch_slot_number}


def matrix_action(field, thermal_inertia):
    padded = jnp.pad(field, 1)
    beside = padded[2:, 1:-1, 1:-1] + padded[:-2, 1:-1, 1:-1]
    beside = beside + padded[1:-1, 2:, 1:-1] + padded[1:-1, :-2, 1:-1]
    beside = beside + padded[1:-1, 1:-1, 2:] + padded[1:-1, 1:-1, :-2]
    return (6.0 + thermal_inertia) * field - beside


def reference(earlier_thermal_state, thermal_inertia, boundary_energy_current, jacobian_quad_factors, patch_holder_liquid, patch_slot_number):
    icells = CX * CY
    rows_index = jnp.arange(ROWS, dtype=jnp.int32)
    device = rows_index // icells
    solid_index = device % N_SOLID
    owner_device = patch_holder_liquid[:, 0].astype(jnp.int32) * N_SOLID + solid_index
    columns = owner_device * FACE_DEV + patch_slot_number.astype(jnp.int32)
    picked = jnp.take(boundary_energy_current, columns, axis=1)
    source = jnp.sum(jacobian_quad_factors * picked, axis=0)
    layer = source.reshape(N_FLUID, N_SOLID, CX, CY).transpose(0, 2, 1, 3).reshape(SOLID_COUNT_X, SOLID_COUNT_Y)
    forcing_entries = thermal_inertia * earlier_thermal_state
    forcing_entries = forcing_entries.at[:, :, SOLID_COUNT_Z - 1].add(layer)
    diagonal = 6.0 + thermal_inertia
    thermal_state_guess = earlier_thermal_state
    equation_misfit = forcing_entries - matrix_action(thermal_state_guess, thermal_inertia)
    precond = equation_misfit / diagonal
    update_course = precond
    norm_now = jnp.sum(equation_misfit * precond)
    for iteration in range(ITERS):
        image = matrix_action(update_course, thermal_inertia)
        update_multiplier = norm_now / jnp.sum(update_course * image)
        thermal_state_guess = thermal_state_guess + update_multiplier * update_course
        equation_misfit = equation_misfit - update_multiplier * image
        precond = equation_misfit / diagonal
        norm_next = jnp.sum(equation_misfit * precond)
        update_course = precond + (norm_next / norm_now) * update_course
        norm_now = norm_next
    return thermal_state_guess, equation_misfit
```

```python
import functools

import jax
import jax.numpy as jnp
from jax import lax
from jax.experimental import pallas as pl
from jax.experimental.pallas import tpu as pltpu
from jax.sharding import PartitionSpec as P

ITERS = 3
XCHIPS = 4
CORES = 2
MESH = pl.DeviceIdType.MESH
F32 = jnp.float32
BF16 = jnp.bfloat16
AROUND = [(a, b) for a in (-1, 0, 1) for b in (-1, 0, 1) if (a, b) != (0, 0)]
LOW = 5
SIDE = 8


def iota(shape, axis):
    return lax.broadcasted_iota(jnp.int32, shape, axis)


def body(
    nx, ny, nz,
    x0_hbm, c_hbm, b_hbm, j_hbm, owner_hbm, slot_hbm,
    guess_hbm, misfit_hbm,
    xe, de, w0, w1, w2, last,
    bv, jv, idx, tabs, held, jac, codes, code_own, key, jm, acc,
    part_out, part_in, source, around_in, sum_out, sum_x, sum_y, sum_z,
    load_sem, store_sem, bx_send, bx_recv, jx_send, jx_recv, cx_send, cx_recv,
    ring_send, ring_recv, halo_send, halo_recv, px_send, px_recv,
    sh_send, sh_recv, ar_send, ar_recv,
):
    cx, cy, cz = (xe.shape[0] - 10, xe.shape[1] - 16, xe.shape[2])
    quads, faces = bv.shape
    rows = jv.shape[1]
    share = quads // nx
    many = 128 // share
    deep = faces // many
    rowsets = rows // 128
    f, s = lax.axis_index("fluid"), lax.axis_index("solid")
    nf, ns = nx * ny, nz * CORES
    x, y = lax.rem(f, nx), f // nx
    core, z = lax.rem(s, CORES), s // CORES

    def remote(src, dst, send, recv, at):
        return pltpu.make_async_remote_copy(
            src_ref=src, dst_ref=dst, send_sem=send, recv_sem=recv,
            device_id=at, device_id_type=MESH,
        )

    def beside(a, b):
        return (lax.rem(f + a + nf, nf), lax.rem(s + b + ns, ns))

    def on_x(d, flip):
        return (y * nx + lax.rem(x + d, nx), z * CORES + lax.rem(core + flip, CORES))

    def on_y(d):
        return (lax.rem(y + d, ny) * nx + x, s)

    def on_z(d):
        return (f, lax.rem(z + d, nz) * CORES + core)

    plane = [(d, flip) for d in range(nx) for flip in range(CORES) if (d, flip) != (0, 0)]

    inner = (pl.ds(LOW, cx), pl.ds(SIDE, cy))
    loads = [
        pltpu.make_async_copy(b_hbm, bv, load_sem.at[0]),
        pltpu.make_async_copy(owner_hbm, idx.at[0], load_sem.at[1]),
        pltpu.make_async_copy(slot_hbm, idx.at[1], load_sem.at[2]),
        pltpu.make_async_copy(j_hbm, jv, load_sem.at[3]),
        pltpu.make_async_copy(x0_hbm, xe.at[inner], load_sem.at[4]),
        pltpu.make_async_copy(c_hbm, de.at[inner], load_sem.at[5]),
    ]
    for load in loads:
        load.start()

    barrier = pltpu.get_barrier_semaphore()
    partners = [on_x(d, flip) for d, flip in plane]
    partners += [on_y(d) for d in range(1, ny)] + [on_z(d) for d in range(1, nz)]
    partners += [beside(a, b) for a, b in AROUND]
    for at in partners:
        pl.semaphore_signal(barrier, inc=1, device_id=at, device_id_type=MESH)

    guard = jnp.zeros(xe.shape[1:], F32)
    for ref in (xe, w0, w1, w2):
        ref[0] = guard
        ref[cx + 9] = guard

    loads[0].wait()
    for a in range(nx):
        mine = bv[a * share : (a + 1) * share, :]
        stack = jnp.concatenate(
            [mine[:, (m * deep // 128) * 128 : (m * deep // 128) * 128 + 128] for m in range(many)], axis=0
        )
        if deep < 128:
            turned = pltpu.roll(stack, 128 - deep, 1)
            odd = (iota(stack.shape, 0) // share) % 2 == 1
            stack = jnp.where(odd, turned, stack)
        tabs[a] = stack.T[:deep]
    loads[1].wait()
    loads[2].wait()
    code_own[...] = idx[0] * faces + idx[1]
    codes[0] = code_own[...]
    held[y, 0] = tabs[x]
    loads[3].wait()
    jac[0] = jv[pl.ds(pl.multiple_of(x * share, share), share), :]
    acc[...] = jnp.zeros_like(acc)
    loads[4].wait()
    loads[5].wait()

    pl.semaphore_wait(barrier, len(partners))

    spread = []
    for d in range(1, nx):
        at = on_x(d, 0)
        to = lax.rem(x + d, nx)
        spread.append(remote(tabs.at[to], held.at[y, d], bx_send.at[d - 1], bx_recv.at[d - 1], at))
        spread[-1].start()

    def ring(t, d, way):
        slot = lax.rem(y + ny + (1 - t if way == 0 else t - 1), ny)
        at = on_y(1 if way == 0 else ny - 1)
        block = held.at[slot, d]
        return remote(block, block, ring_send.at[way, t - 1, d], ring_recv.at[way, t - 1, d], at)

    half = ny // 2

    def goes(t, d, way):
        return t < half or (d < nx // 2) == (way == 0)

    ways = [
        [[ring(t, d, way) if goes(t, d, way) else None for way in range(2)] for d in range(nx)]
        for t in range(1, half + 1)
    ]

    def forward(t, d):
        if t == 1:
            if d > 0:
                spread[d - 1].wait_recv()
        else:
            for way in range(2):
                ways[t - 2][d][way].wait_recv()
        for way in range(2):
            if goes(t, d, way):
                ways[t - 1][d][way].start()

    forward(1, 0)
    coded, jacs, halos = [], [], []
    for d in range(1, nx):
        at, to = on_x(d, 0), lax.rem(x + d, nx)
        coded.append(remote(code_own, codes.at[d], cx_send.at[d - 1], cx_recv.at[d - 1], at))
        coded[-1].start()
        jacs.append(
            remote(
                jv.at[pl.ds(pl.multiple_of(to * share, share), share)], jac.at[d],
                jx_send.at[d - 1], jx_recv.at[d - 1], at,
            )
        )
        jacs[-1].start()
    to_x = {-1: (pl.ds(LOW, 4), pl.ds(LOW + cx, 4)), 0: (pl.ds(LOW, cx),) * 2, 1: (pl.ds(LOW + cx - 4, 4), pl.ds(LOW - 4, 4))}
    to_y = {-1: (pl.ds(SIDE, 8), pl.ds(SIDE + cy, 8)), 0: (pl.ds(SIDE, cy),) * 2, 1: (pl.ds(SIDE + cy - 8, 8), pl.ds(SIDE - 8, 8))}
    for n, (a, b) in enumerate(AROUND):
        for k, ref in enumerate((xe, de)):
            halos.append(
                remote(
                    ref.at[to_x[a][0], to_y[b][0]], ref.at[to_x[a][1], to_y[b][1]],
                    halo_send.at[k, n], halo_recv.at[k, n], beside(a, b),
                )
            )
            halos[-1].start()
    for d in range(1, nx):
        forward(1, d)

    def prepare(d):
        if d > 0:
            coded[d - 1].wait_recv()
            jacs[d - 1].wait_recv()

        def one(i, carry):
            code = codes[d, pl.ds(i, 1), :]
            place = pl.ds(pl.multiple_of(d * rows + i * 128, 128), 128)
            owner, slot = code // faces, lax.rem(code, faces)
            keys = (owner * deep + lax.rem(slot, deep)).astype(F32)
            key[place, :] = jnp.broadcast_to(keys, (128, 128)).T
            j = jac[d, :, pl.ds(pl.multiple_of(i * 128, 128), 128)]
            tiled = jnp.concatenate([j] * many, axis=0)
            wanted = iota((128, 128), 0) // share == jnp.broadcast_to(slot // deep, (128, 128))
            jm[place, :] = jnp.where(wanted, tiled, 0.0).T
            return carry

        lax.fori_loop(0, rowsets, one, 0)

    lane_f = iota((256, 128), 1).astype(F32)

    def weight(slot):
        parts = []
        for d in range(nx):
            parts.append(held[slot, d])
        table = jnp.concatenate(parts, axis=0)
        high = table.astype(BF16)
        low = (table - high.astype(F32)).astype(BF16)
        return jnp.concatenate([high, low], axis=1)

    def base_of(slot, d):
        return (slot * nx + lax.rem(x - d + nx, nx)) * deep

    def pick(d, slots):
        tables = [weight(slot) for slot in slots]
        lanes = iota((1, 128), 1)
        marks = []
        for slot in slots:
            for tile in range(nx * deep // 128):
                mark = jnp.zeros((1, 128), jnp.int32)
                for e in range(128 // deep):
                    p = tile * (128 // deep) + e
                    mark = jnp.where(lanes // deep == e, base_of(slot, p) + lanes - e * deep, mark)
                marks.append(jnp.broadcast_to(mark.astype(F32), (256, 128)))

        def one(i, carry):
            place = pl.ds(pl.multiple_of(d * rows + i * 256, 256), 256)
            keys = key[place, :]
            got = acc[place, :]
            per = len(marks) // len(slots)
            for n, table in enumerate(tables):
                hot = jnp.concatenate(
                    [jnp.where(keys == mark, 1.0, 0.0).astype(BF16) for mark in marks[n * per : (n + 1) * per]],
                    axis=1,
                )
                both = jnp.dot(hot, table, preferred_element_type=F32)
                got = got + (both[:, :128] + both[:, 128:])
            acc[place, :] = got
            return carry

        lax.fori_loop(0, rows // 256, one, 0)

    def around_sum(ref, r, n):
        mid = ref[pl.ds(r, n)].reshape(n * xe.shape[1], cz)
        out = ref[pl.ds(r - 1, n)] + ref[pl.ds(r + 1, n)]
        out = out.reshape(n * xe.shape[1], cz)
        out = out + (pltpu.roll(mid, 1, 0) + pltpu.roll(mid, mid.shape[0] - 1, 0))
        lane = iota(mid.shape, 1)
        out = out + jnp.where(lane == 0, 0.0, pltpu.roll(mid, 1, 1))
        out = out + jnp.where(lane == cz - 1, 0.0, pltpu.roll(mid, cz - 1, 1))
        return out.reshape(n, xe.shape[1], cz)

    def start_solid():
        for halo in halos:
            halo.wait_recv()
        for ref, fill in ((xe, 0.0), (de, 1e30)):
            @pl.when(f == 0)
            def _():
                ref[pl.ds(LOW - 4, 4)] = jnp.full((4,) + xe.shape[1:], fill, F32)

            @pl.when(f == nf - 1)
            def _():
                ref[pl.ds(LOW + cx, 4)] = jnp.full((4,) + xe.shape[1:], fill, F32)

            @pl.when(s == 0)
            def _():
                ref[pl.ds(1, cx + 8), pl.ds(0, 8)] = jnp.full((cx + 8, 8, cz), fill, F32)

            @pl.when(s == ns - 1)
            def _():
                ref[pl.ds(1, cx + 8), pl.ds(SIDE + cy, 8)] = jnp.full((cx + 8, 8, cz), fill, F32)

        def one(i, carry):
            r = 1 + 8 * i
            got = around_sum(xe, r, 8) - 6.0 * xe[pl.ds(r, 8)]
            c = de[pl.ds(r, 8)]
            inverse = jnp.where(c > 1e29, 0.0, 1.0 / (6.0 + c))
            de[pl.ds(r, 8)] = inverse
            w0[pl.ds(r, 8)] = inverse * got
            return carry

        lax.fori_loop(0, (cx + 8) // 8, one, 0)

    for halo in halos:
        halo.wait_send()
    start_solid()
    for d in range(nx):
        prepare(d)
    for t in range(2, half + 1):
        far = t - 2
        slots = [y] if far == 0 else [lax.rem(y + ny - far, ny), lax.rem(y + far, ny)]
        for d in range(nx):
            forward(t, d)
            pick(d, slots)
    far = half - 1
    slots = [y] if far == 0 else [lax.rem(y + ny - far, ny), lax.rem(y + far, ny)]
    for d in range(nx):
        pick(d, slots)
    for d in range(nx):
        for way in range(2):
            if goes(half, d, way):
                ways[half - 1][d][way].wait_recv()
    for d in range(nx):
        pick(d, [lax.rem(y + half, ny)])

        def one(i, carry):
            place = pl.ds(pl.multiple_of(d * rows + i * 128, 128), 128)
            product = acc[place, :] * jm[place, :]
            part_out[d, pl.ds(i, 1), :] = jnp.sum(product.T, axis=0, keepdims=True)
            return carry

        lax.fori_loop(0, rowsets, one, 0)
    parts = []
    for d in range(1, nx):
        parts.append(
            remote(part_out.at[d], part_in.at[d - 1], px_send.at[d - 1], px_recv.at[d - 1], on_x(nx - d, 0))
        )
        parts[-1].start()
    total = part_out[0]
    for d in range(1, nx):
        parts[d - 1].wait_recv()
    for d in range(1, nx):
        total = total + part_in[d - 1]
    source[...] = total

    shared = []
    for n, (a, b) in enumerate(AROUND):
        shared.append(remote(source, around_in.at[n], sh_send.at[n], sh_recv.at[n], beside(a, b)))
        shared[-1].start()

    def heat(r, first, n, line, offset):
        spot = iota((n, 128), 1)
        column = jnp.where(spot == iota((n, 128), 0) + offset, jnp.broadcast_to(line, (n, 128)), 0.0)
        column = jnp.sum(column, axis=1, keepdims=True)
        w0[r, pl.ds(first, n), :] += jnp.where(spot == cz - 1, column * de[r, pl.ds(first, n), :], 0.0)

    per = 128 // cy

    def heat_inner(i, carry):
        line = source[pl.ds(i, 1), :]
        for k in range(per):
            heat(LOW + i * per + k, SIDE, cy, line, k * cy)
        return carry

    lax.fori_loop(0, cx // per, heat_inner, 0)
    for n, (a, b) in enumerate(AROUND):
        shared[n].wait_recv()
    for n, (a, b) in enumerate(AROUND):
        first = {0: SIDE, 1: 0, -1: SIDE + cy}[b]
        count = {0: cy, 1: 8, -1: 8}[b]
        offset = {0: 0, 1: cy - 8, -1: 0}[b]
        if a == 0:
            def heat_side(i, carry, n=n, first=first, count=count, offset=offset):
                line = around_in[n, pl.ds(i, 1), :]
                for k in range(per):
                    heat(LOW + i * per + k, first, count, line, k * cy + offset)
                return carry

            lax.fori_loop(0, cx // per, heat_side, 0)
        else:
            line = around_in[n, cx // per - 1 : cx // per, :] if a == 1 else around_in[n, 0:1, :]
            for k in range(per):
                heat((1 if a == 1 else LOW + cx) + k, first, count, line, k * cy + offset)

    def fold(v):
        return jnp.sum(v.reshape(-1, 8, cz), axis=0)

    def inside(v):
        return v[:, SIDE : SIDE + cy]

    def step(ref, new, first):
        def one(i, carry):
            r = LOW + 8 * i
            near = around_sum(ref, r, 8)
            inverse = de[pl.ds(r, 8)]
            new_w = inverse * near
            new[pl.ds(r, 8)] = new_w
            now = inside(ref[pl.ds(r, 8)])
            near = inside(near)
            odd = carry[0] + fold(now * near)
            even = carry[1] + fold(inside(new_w) * near)
            if first:
                return (odd, even, carry[2] + fold(now * now / inside(inverse)))
            return (odd, even)

        zero = jnp.zeros((8, cz), F32)
        sums = lax.fori_loop(0, cx // 8, one, (zero,) * (3 if first else 2))
        for r in (LOW - 4, LOW + cx):
            new[pl.ds(r, 4)] = de[pl.ds(r, 4)] * around_sum(ref, r, 4)
        return sums

    mu1, mu2, mu0 = step(w0, w1, True)
    mu3, mu4 = step(w1, w2, False)

    def final(i, carry):
        near = inside(around_sum(w2, LOW + 8 * i, 8))
        last[pl.ds(8 * i, 8)] = near
        return carry + fold(inside(w2[pl.ds(LOW + 8 * i, 8)]) * near)

    mu5 = lax.fori_loop(0, cx // 8, final, jnp.zeros((8, cz), F32))
    lines = [jnp.sum(v, axis=0, keepdims=True) for v in (mu0, mu1, mu2, mu3, mu4, mu5)]
    lines.append(jnp.zeros((2, cz), F32))
    local = jnp.concatenate(lines, axis=0)

    sends = []

    def reduce(stage, value, slots, me, peers):
        sum_out[stage] = value
        slots[me] = value
        copies = []
        for n, at in enumerate(peers):
            copies.append(
                remote(sum_out.at[stage], slots.at[me], ar_send.at[stage, n], ar_recv.at[stage, n], at)
            )
            copies[-1].start()
        for copy in copies:
            copy.wait_recv()
        sends.extend(copies)
        return jnp.sum(slots[...], axis=0)

    local = reduce(0, local, sum_x, x * CORES + core, [on_x(d, flip) for d, flip in plane])
    local = reduce(1, local, sum_y, y, [on_y(d) for d in range(1, ny)])
    local = reduce(2, local, sum_z, z, [on_z(d) for d in range(1, nz)])
    total = jnp.broadcast_to(jnp.sum(local, axis=1, keepdims=True), (8, cz))
    mu = [total[k : k + 1] for k in range(6)]

    def product(u, v):
        out = 0.0
        for a, left in enumerate(u):
            for b, right in enumerate(v):
                out = out + left * right * mu[a + b]
        return out

    one_line = jnp.ones((1, cz), F32)
    course, misfit, guess = [one_line], [one_line], []
    rz = mu[0]
    for it in range(ITERS):
        image = [
            (course[k] if k < len(course) else 0.0) - (course[k - 1] if k > 0 else 0.0)
            for k in range(len(course) + 1)
        ]
        alpha = rz / product(course, image)
        guess = [(guess[k] if k < len(guess) else 0.0) + alpha * course[k] for k in range(len(course))]
        misfit = [(misfit[k] if k < len(misfit) else 0.0) - alpha * image[k] for k in range(len(image))]
        if it + 1 < ITERS:
            new = product(misfit, misfit)
            ratio = new / rz
            course = [misfit[k] + (ratio * course[k] if k < len(course) else 0.0) for k in range(len(misfit))]
            rz = new

    def combine(i, carry):
        here = (pl.ds(LOW + 4 * i, 4), pl.ds(SIDE, cy))
        basis = [w0[here], w1[here], w2[here]]
        step_sum, rest = 0.0, 0.0
        for k in range(3):
            step_sum = step_sum + guess[k] * basis[k]
            rest = rest + misfit[k] * basis[k]
        xe[here] = xe[here] + step_sum
        spot = pl.ds(4 * i, 4)
        last[spot] = rest / de[here] + misfit[3] * last[spot]
        return carry

    lax.fori_loop(0, cx // 4, combine, 0)
    stores = [
        pltpu.make_async_copy(xe.at[inner], guess_hbm, store_sem.at[0]),
        pltpu.make_async_copy(last, misfit_hbm, store_sem.at[1]),
    ]
    for store in stores:
        store.start()
    for copy in spread + coded + jacs + parts + shared + sends:
        copy.wait_send()
    for t in range(1, half + 1):
        for d in range(nx):
            for way in range(2):
                if goes(t, d, way):
                    ways[t - 1][d][way].wait_send()
    for store in stores:
        store.wait()


def per_device(nx, ny, nz, x0, c, b, j, owner, slot):
    quads, faces = b.shape
    rows = slot.shape[0]
    cx, cy, cz = x0.shape
    share = quads // nx
    deep = faces * share // 128
    half = ny // 2
    wide = (cx + 10, cy + 16, cz)
    lines = rows // 128
    dma = pltpu.SemaphoreType.DMA
    vmem = pltpu.VMEM
    peers = max(nx * CORES, ny, nz)
    scratch = [
        vmem(wide, F32), vmem(wide, F32), vmem(wide, F32), vmem(wide, F32), vmem(wide, F32), vmem((cx, cy, cz), F32),
        vmem((quads, faces), F32), vmem((quads, rows), F32), vmem((2, lines, 128), jnp.int32),
        vmem((nx, deep, 128), F32), vmem((ny, nx, deep, 128), F32), vmem((nx, share, rows), F32),
        vmem((nx, lines, 128), jnp.int32), vmem((lines, 128), jnp.int32),
        vmem((nx * rows, 128), F32), vmem((nx * rows, 128), F32), vmem((nx * rows, 128), F32),
        vmem((nx, lines, 128), F32), vmem((nx - 1, lines, 128), F32), vmem((lines, 128), F32),
        vmem((8, lines, 128), F32), vmem((3, 8, 128), F32),
        vmem((nx * CORES, 8, 128), F32), vmem((ny, 8, 128), F32), vmem((nz, 8, 128), F32),
        dma((6,)), dma((2,)), dma((nx - 1,)), dma((nx - 1,)), dma((nx - 1,)), dma((nx - 1,)), dma((nx - 1,)), dma((nx - 1,)),
        dma((2, half, nx)), dma((2, half, nx)), dma((2, 8)), dma((2, 8)), dma((nx - 1,)), dma((nx - 1,)),
        dma((8,)), dma((8,)), dma((3, peers)), dma((3, peers)),
    ]
    out = jax.ShapeDtypeStruct((cx, cy, cz), F32)
    anywhere = pl.BlockSpec(memory_space=pl.ANY)
    return pl.pallas_call(
        functools.partial(body, nx, ny, nz),
        out_shape=(out, out),
        in_specs=[anywhere] * 6,
        out_specs=(anywhere, anywhere),
        scratch_shapes=scratch,
        compiler_params=pltpu.CompilerParams(collective_id=0, has_side_effects=True, vmem_limit_bytes=40 * 2**20),
        name="coupling_step",
    )(x0, c, b, j, owner.reshape(lines, 128), slot.reshape(lines, 128))


def solution(mesh):
    nx, nz = XCHIPS, mesh.shape["solid"] // CORES
    ny = mesh.shape["fluid"] // nx
    both = ("fluid", "solid")
    block = P("fluid", "solid", None)
    return jax.shard_map(
        functools.partial(per_device, nx, ny, nz),
        mesh=mesh,
        in_specs=(block, block, P(None, both), P(None, both), P(both, None), P(both)),
        out_specs=(block, block),
        check_vma=False,
    )
```

```python
import functools

import jax
import jax.numpy as jnp
from jax import lax
from jax.experimental import pallas as pl
from jax.experimental.pallas import tpu as pltpu
from jax.sharding import PartitionSpec as P

ITERS = 3
XCHIPS = 4
CORES = 2
MESH = pl.DeviceIdType.MESH
F32 = jnp.float32
BF16 = jnp.bfloat16
AROUND = [(a, b) for a in (-1, 0, 1) for b in (-1, 0, 1) if (a, b) != (0, 0)]
LOW = 5
SIDE = 8


def iota(shape, axis):
    return lax.broadcasted_iota(jnp.int32, shape, axis)


def body(
    nx, ny, nz,
    x0_hbm, c_hbm, b_hbm, j_hbm, owner_hbm, slot_hbm,
    xe, de, w0, w1, w2, last, coefs,
    bv, jv, idx, tabs, held, jac, codes, code_own, key, jm, acc,
    part_out, part_in, source, around_in, sum_out, sum_plane, sum_line,
    load_sem, bx_send, bx_recv, jx_send, jx_recv, cx_send, cx_recv,
    ring_send, ring_recv, halo_send, halo_recv, px_send, px_recv,
    sh_send, sh_recv, ar_send, ar_recv,
):
    cx, cy, cz = (xe.shape[0] - 10, xe.shape[1] - 16, xe.shape[2])
    quads, faces = bv.shape
    rows = jv.shape[1]
    share = quads // nx
    many = 128 // share
    deep = faces // many
    rowsets = rows // 128
    f, s = lax.axis_index("fluid"), lax.axis_index("solid")
    nf, ns = nx * ny, nz * CORES
    x, y = lax.rem(f, nx), f // nx

    def remote(src, dst, send, recv, at):
        return pltpu.make_async_remote_copy(
            src_ref=src, dst_ref=dst, send_sem=send, recv_sem=recv,
            device_id=at, device_id_type=MESH,
        )

    def beside(a, b):
        return (lax.rem(f + a + nf, nf), lax.rem(s + b + ns, ns))

    def on_x(d):
        return (y * nx + lax.rem(x + d, nx), s)

    def on_y(d):
        return (lax.rem(y + d, ny) * nx + x, s)

    def on_plane(n):
        return (lax.rem(f + n, nf), s)

    def on_line(n):
        return (f, lax.rem(s + n, ns))

    inner = (pl.ds(LOW, cx), pl.ds(SIDE, cy))
    loads = [
        pltpu.make_async_copy(b_hbm, bv, load_sem.at[0]),
        pltpu.make_async_copy(owner_hbm, idx.at[0], load_sem.at[1]),
        pltpu.make_async_copy(slot_hbm, idx.at[1], load_sem.at[2]),
        pltpu.make_async_copy(j_hbm, jv, load_sem.at[3]),
        pltpu.make_async_copy(x0_hbm, xe.at[inner], load_sem.at[4]),
        pltpu.make_async_copy(c_hbm, de.at[inner], load_sem.at[5]),
    ]
    for load in loads:
        load.start()

    barrier = pltpu.get_barrier_semaphore()
    partners = [on_x(d) for d in range(1, nx)] + [on_line(n) for n in range(1, ns)]
    partners += [on_y(1), on_y(ny - 1)] + [beside(a, b) for a, b in AROUND if a != 0]
    for at in partners:
        pl.semaphore_signal(barrier, inc=1, device_id=at, device_id_type=MESH)

    guard = jnp.zeros(xe.shape[1:], F32)
    for ref in (xe, w0, w1, w2):
        ref[0] = guard
        ref[cx + 9] = guard

    with jax.named_scope("tables"):
        loads[0].wait()
        for a in range(nx):
            mine = bv[a * share : (a + 1) * share, :]
            stack = jnp.concatenate(
                [mine[:, (m * deep // 128) * 128 : (m * deep // 128) * 128 + 128] for m in range(many)], axis=0
            )
            if deep < 128:
                turned = pltpu.roll(stack, 128 - deep, 1)
                odd = (iota(stack.shape, 0) // share) % 2 == 1
                stack = jnp.where(odd, turned, stack)
            tabs[a] = stack.T[:deep]
        loads[1].wait()
        loads[2].wait()
        code_own[...] = idx[0] * faces + idx[1]
        codes[0] = code_own[...]
        held[y, 0] = tabs[x]
        loads[3].wait()
        jac[0] = jv[pl.ds(pl.multiple_of(x * share, share), share), :]
        loads[4].wait()
        loads[5].wait()

    with jax.named_scope("entry"):
        pl.semaphore_wait(barrier, len(partners))

    spread, coded, jacs, halos = [], [], [], []
    for d in range(1, nx):
        coded.append(remote(code_own, codes.at[d], cx_send.at[d - 1], cx_recv.at[d - 1], on_x(d)))
        coded[-1].start()
    for d in range(1, nx):
        to = lax.rem(x + d, nx)
        spread.append(remote(tabs.at[to], held.at[y, d], bx_send.at[d - 1], bx_recv.at[d - 1], on_x(d)))
        spread[-1].start()

    def ring(t, d, way):
        slot = lax.rem(y + ny + (1 - t if way == 0 else t - 1), ny)
        at = on_y(1 if way == 0 else ny - 1)
        block = held.at[slot, d]
        return remote(block, block, ring_send.at[way, t - 1, d], ring_recv.at[way, t - 1, d], at)

    half = ny // 2

    def goes(t, d, way):
        return t < half or (d < nx // 2) == (way == 0)

    ways = [
        [[ring(t, d, way) if goes(t, d, way) else None for way in range(2)] for d in range(nx)]
        for t in range(1, half + 1)
    ]

    def forward(t, d):
        if t == 1 and d > 0:
            spread[d - 1].wait_recv()
        for way in range(2):
            if t > 1:
                ways[t - 2][d][way].wait_recv()
            if goes(t, d, way):
                ways[t - 1][d][way].start()

    forward(1, 0)
    def prepare_keys(d):
        if d > 0:
            coded[d - 1].wait_recv()
        for i in range(rowsets):
            code = codes[d, i : i + 1, :]
            owner, slot = code // faces, lax.rem(code, faces)
            keys = (owner * deep + lax.rem(slot, deep)).astype(F32)
            key[d * rows + i * 128 : d * rows + (i + 1) * 128, :] = jnp.broadcast_to(keys, (128, 128)).T

    def prepare_jac(d):
        if d > 0:
            jacs[d - 1].wait_recv()
        for i in range(rowsets):
            slot = lax.rem(codes[d, i : i + 1, :], faces)
            j = jac[d, :, i * 128 : (i + 1) * 128]
            tiled = jnp.concatenate([j] * many, axis=0)
            wanted = iota((128, 128), 0) // share == jnp.broadcast_to(slot // deep, (128, 128))
            jm[d * rows + i * 128 : d * rows + (i + 1) * 128, :] = jnp.where(wanted, tiled, 0.0).T

    def weight(slot):
        parts = []
        for d in range(nx):
            parts.append(held[slot, d])
        table = jnp.concatenate(parts, axis=0)
        high = table.astype(BF16)
        low = (table - high.astype(F32)).astype(BF16)
        return jnp.concatenate([high, low], axis=1)

    def base_of(slot, d):
        return (slot * nx + lax.rem(x - d + nx, nx)) * deep

    tall = 512

    def pick(d, slots, first=False, finish=False):
        table = jnp.concatenate([weight(slot) for slot in slots], axis=0)
        lanes = iota((1, 128), 1)
        marks = []
        for slot in slots:
            for tile in range(nx * deep // 128):
                mark = jnp.zeros((1, 128), jnp.int32)
                for e in range(128 // deep):
                    p = tile * (128 // deep) + e
                    mark = jnp.where(lanes // deep == e, base_of(slot, p) + lanes - e * deep, mark)
                marks.append(mark.astype(F32))
        for i in range(rows // tall):
            place = pl.ds(d * rows + i * tall, tall)
            keys = key[place, :]
            hot = jnp.concatenate([jnp.where(keys == mark, 1.0, 0.0).astype(BF16) for mark in marks], axis=1)
            both = jnp.dot(hot, table, preferred_element_type=F32)
            got = both[:, :128] + both[:, 128:]
            if not first:
                got = got + acc[place, :]
            if not finish:
                acc[place, :] = got
                continue
            product = got * jm[place, :]
            for k in range(tall // 128):
                line = jnp.sum(product[k * 128 : (k + 1) * 128].T, axis=0, keepdims=True)
                at = i * (tall // 128) + k
                part_out[d, at : at + 1, :] = line

    def around_sum(ref, r, n):
        mid = ref[pl.ds(r, n)].reshape(n * xe.shape[1], cz)
        out = ref[pl.ds(r - 1, n)] + ref[pl.ds(r + 1, n)]
        out = out.reshape(n * xe.shape[1], cz)
        out = out + (pltpu.roll(mid, 1, 0) + pltpu.roll(mid, mid.shape[0] - 1, 0))
        lane = iota(mid.shape, 1)
        out = out + jnp.where(lane == 0, 0.0, pltpu.roll(mid, 1, 1))
        out = out + jnp.where(lane == cz - 1, 0.0, pltpu.roll(mid, cz - 1, 1))
        return out.reshape(n, xe.shape[1], cz)

    def start_solid():
        for ref, fill in ((xe, 0.0), (de, 1e30)):
            @pl.when(f == 0)
            def _():
                ref[pl.ds(LOW - 4, 4)] = jnp.full((4,) + xe.shape[1:], fill, F32)

            @pl.when(f == nf - 1)
            def _():
                ref[pl.ds(LOW + cx, 4)] = jnp.full((4,) + xe.shape[1:], fill, F32)

            @pl.when(s == 0)
            def _():
                ref[pl.ds(1, cx + 8), pl.ds(0, 8)] = jnp.full((cx + 8, 8, cz), fill, F32)

            @pl.when(s == ns - 1)
            def _():
                ref[pl.ds(1, cx + 8), pl.ds(SIDE + cy, 8)] = jnp.full((cx + 8, 8, cz), fill, F32)

        def one(i, carry):
            r = 1 + 8 * i
            got = around_sum(xe, r, 8) - 6.0 * xe[pl.ds(r, 8)]
            c = de[pl.ds(r, 8)]
            inverse = jnp.where(c > 1e29, 0.0, 1.0 / (6.0 + c))
            de[pl.ds(r, 8)] = inverse
            w0[pl.ds(r, 8)] = inverse * got
            return carry

        lax.fori_loop(0, (cx + 8) // 8, one, 0)

    order = sorted(range(nx), key=lambda d: (min(d, nx - d), -d))
    for d in order:
        if d > 0:
            with jax.named_scope(f"forward#t=1#d={d}"):
                forward(1, d)
        with jax.named_scope(f"prepare_keys#d={d}"):
            prepare_keys(d)

    for d in range(1, nx):
        to = lax.rem(x + d, nx)
        jacs.append(
            remote(
                jv.at[pl.ds(pl.multiple_of(to * share, share), share)], jac.at[d],
                jx_send.at[d - 1], jx_recv.at[d - 1], on_x(d),
            )
        )
        jacs[-1].start()
    to_x = {-1: (pl.ds(LOW, 4), pl.ds(LOW + cx, 4)), 0: (pl.ds(LOW, cx),) * 2, 1: (pl.ds(LOW + cx - 4, 4), pl.ds(LOW - 4, 4))}
    to_y = {-1: (pl.ds(SIDE, 8), pl.ds(SIDE + cy, 8)), 0: (pl.ds(SIDE, cy),) * 2, 1: (pl.ds(SIDE + cy - 8, 8), pl.ds(SIDE - 8, 8))}
    def send_halos(chosen):
        for n in chosen:
            a, b = AROUND[n]
            for k, ref in enumerate((xe, de)):
                halos.append(
                    remote(
                        ref.at[to_x[a][0], to_y[b][0]], ref.at[to_x[a][1], to_y[b][1]],
                        halo_send.at[k, n], halo_recv.at[k, n], beside(a, b),
                    )
                )
                halos[-1].start()

    send_halos([n for n, (a, b) in enumerate(AROUND) if a == 0])

    def near(far):
        if far == 0:
            return [y]
        return [lax.rem(y + ny - far, ny), lax.rem(y + far, ny)]

    for t in range(2, half + 1):
        for d in order:
            with jax.named_scope(f"forward#t={t}#d={d}"):
                forward(t, d)
            with jax.named_scope(f"pick#t={t}#d={d}"):
                pick(d, near(t - 2), first=t == 2)
            if t == half:
                with jax.named_scope(f"prepare_jac#d={d}"):
                    prepare_jac(d)
    send_halos([n for n, (a, b) in enumerate(AROUND) if a != 0])
    if half == 1:
        for d in range(nx):
            prepare_jac(d)
    for d in range(nx):
        with jax.named_scope(f"pick_near#d={d}"):
            pick(d, near(half - 1), first=half == 1)
    with jax.named_scope("far_wait"):
        for d in range(nx):
            for way in range(2):
                if goes(half, d, way):
                    ways[half - 1][d][way].wait_recv()
    parts = {}
    for d in list(range(1, nx)) + [0]:
        with jax.named_scope(f"pick_far#d={d}"):
            pick(d, [lax.rem(y + half, ny)], finish=True)
        if d > 0:
            parts[d] = remote(part_out.at[d], part_in.at[d - 1], px_send.at[d - 1], px_recv.at[d - 1], on_x(nx - d))
            parts[d].start()
    with jax.named_scope("solid_wait"):
        for halo in halos:
            halo.wait_send()
        for halo in halos:
            halo.wait_recv()
    with jax.named_scope("solid_start"):
        start_solid()
    total = part_out[0]
    with jax.named_scope("part_wait"):
        for d in range(1, nx):
            parts[d].wait_recv()
    for d in range(1, nx):
        total = total + part_in[d - 1]
    source[...] = total

    shared = []
    for n, (a, b) in enumerate(AROUND):
        shared.append(remote(source, around_in.at[n], sh_send.at[n], sh_recv.at[n], beside(a, b)))
        shared[-1].start()

    per = 128 // cy

    def heat(r, first, count, line, offset):
        shape = (per, count, 128)
        spot = iota(shape, 2)
        picked = jnp.where(spot == iota(shape, 0) * cy + iota(shape, 1) + offset, line.reshape(1, 1, 128), 0.0)
        column = jnp.sum(picked, axis=2, keepdims=True)
        here = (pl.ds(r, per), pl.ds(first, count))
        w0[here] = w0[here] + jnp.where(spot == cz - 1, column * de[here], 0.0)

    with jax.named_scope("heat_inner"):
        for i in range(cx // per):
            heat(LOW + i * per, SIDE, cy, source[i : i + 1, :], 0)
    with jax.named_scope("around_wait"):
        for n in range(len(AROUND)):
            shared[n].wait_recv()
    with jax.named_scope("heat_sides"):
        for n, (a, b) in enumerate(AROUND):
            first = {0: SIDE, 1: 0, -1: SIDE + cy}[b]
            count = {0: cy, 1: 8, -1: 8}[b]
            offset = {0: 0, 1: cy - 8, -1: 0}[b]
            spots = {0: range(cx // per), 1: [cx // per - 1], -1: [0]}[a]
            for i in spots:
                r = {0: LOW + i * per, 1: 1, -1: LOW + cx}[a]
                heat(r, first, count, around_in[n, i : i + 1, :], offset)

    def fold(v):
        return jnp.sum(v.reshape(-1, 8, cz), axis=0)

    def inside(v):
        return v[:, SIDE : SIDE + cy]

    def step(ref, new, first):
        def one(i, carry):
            r = LOW + 8 * i
            near = around_sum(ref, r, 8)
            inverse = de[pl.ds(r, 8)]
            new_w = inverse * near
            new[pl.ds(r, 8)] = new_w
            now = inside(ref[pl.ds(r, 8)])
            near = inside(near)
            odd = carry[0] + fold(now * near)
            even = carry[1] + fold(inside(new_w) * near)
            if first:
                return (odd, even, carry[2] + fold(now * now / inside(inverse)))
            return (odd, even)

        zero = jnp.zeros((8, cz), F32)
        sums = lax.fori_loop(0, cx // 8, one, (zero,) * (3 if first else 2))
        for r in (LOW - 4, LOW + cx):
            new[pl.ds(r, 4)] = de[pl.ds(r, 4)] * around_sum(ref, r, 4)
        return sums

    with jax.named_scope("step#k=0"):
        mu1, mu2, mu0 = step(w0, w1, True)
    with jax.named_scope("step#k=1"):
        mu3, mu4 = step(w1, w2, False)

    def final(i, carry):
        near = inside(around_sum(w2, LOW + 8 * i, 8))
        last[pl.ds(8 * i, 8)] = near
        return carry + fold(inside(w2[pl.ds(LOW + 8 * i, 8)]) * near)

    with jax.named_scope("step#k=2"):
        mu5 = lax.fori_loop(0, cx // 8, final, jnp.zeros((8, cz), F32))
    lines = [jnp.sum(v, axis=0, keepdims=True) for v in (mu0, mu1, mu2, mu3, mu4, mu5)]
    lines.append(jnp.zeros((2, cz), F32))
    sums = jnp.sum(jnp.concatenate(lines, axis=0), axis=1, keepdims=True)
    local = jnp.sum(jnp.where(iota((8, 128), 0) == iota((8, 128), 1), sums, 0.0), axis=0, keepdims=True)
    sends = []

    def reduce(stage, value, slots, me, peers):
        sum_out[stage] = value
        slots[me] = value
        for at in peers:
            remote(sum_out.at[stage], slots.at[me], ar_send.at[stage], ar_recv.at[stage], at).start()
        every = slots.at[pl.ds(0, len(peers))]
        everyone = remote(every, every, ar_send.at[stage], ar_recv.at[stage], peers[0])
        everyone.wait_recv()
        sends.append(everyone)
        return jnp.sum(slots[...], axis=0)

    with jax.named_scope("reduce#k=0"):
        local = reduce(0, local, sum_plane, f, [on_plane(n) for n in range(1, nf)])
    with jax.named_scope("reduce#k=1"):
        local = reduce(1, local, sum_line, s, [on_line(n) for n in range(1, ns)])
    lane = iota((1, 128), 1)
    mu = [jnp.sum(jnp.where(lane == k, local, 0.0), axis=1, keepdims=True) for k in range(6)]
    mu = [jnp.broadcast_to(m, (1, 128)) for m in mu]

    def product(u, v):
        out = 0.0
        for a, left in enumerate(u):
            for b, right in enumerate(v):
                out = out + left * right * mu[a + b]
        return out

    one_line = jnp.ones((1, cz), F32)
    course, misfit, guess = [one_line], [one_line], []
    rz = mu[0]
    for it in range(ITERS):
        image = [
            (course[k] if k < len(course) else 0.0) - (course[k - 1] if k > 0 else 0.0)
            for k in range(len(course) + 1)
        ]
        alpha = rz / product(course, image)
        guess = [(guess[k] if k < len(guess) else 0.0) + alpha * course[k] for k in range(len(course))]
        misfit = [(misfit[k] if k < len(misfit) else 0.0) - alpha * image[k] for k in range(len(image))]
        if it + 1 < ITERS:
            new = product(misfit, misfit)
            ratio = new / rz
            course = [misfit[k] + (ratio * course[k] if k < len(course) else 0.0) for k in range(len(misfit))]
            rz = new

    coefs[...] = jnp.concatenate(guess + misfit + [one_line], axis=0)
    with jax.named_scope("sent"):
        for copy in spread + coded + jacs + list(parts.values()) + shared + sends:
            copy.wait_send()
        for t in range(1, half + 1):
            for d in range(nx):
                for way in range(2):
                    if goes(t, d, way):
                        ways[t - 1][d][way].wait_send()


def finish(xe, de, w0, w1, w2, last, coefs, guess, misfit):
    n, cy, _ = guess.shape
    first = pl.program_id(0) * n
    here = (pl.ds(LOW + first, n), pl.ds(SIDE, cy))
    line = [coefs[k : k + 1, :] for k in range(7)]
    basis = [w0[here], w1[here], w2[here]]
    guess[...] = xe[here] + (line[0] * basis[0] + (line[1] * basis[1] + line[2] * basis[2]))
    rest = line[3] * basis[0] + (line[4] * basis[1] + line[5] * basis[2])
    misfit[...] = rest / de[here] + line[6] * last[pl.ds(first, n)]


def per_device(nx, ny, nz, x0, c, b, j, owner, slot):
    quads, faces = b.shape
    rows = slot.shape[0]
    cx, cy, cz = x0.shape
    share = quads // nx
    deep = faces * share // 128
    half = ny // 2
    wide = (cx + 10, cy + 16, cz)
    lines = rows // 128
    nf, ns = nx * ny, nz * CORES
    dma = pltpu.SemaphoreType.DMA
    vmem = pltpu.VMEM
    scratch = [
        vmem((quads, faces), F32), vmem((quads, rows), F32), vmem((2, lines, 128), jnp.int32),
        vmem((nx, deep, 128), F32), vmem((ny, nx, deep, 128), F32), vmem((nx, share, rows), F32),
        vmem((nx, lines, 128), jnp.int32), vmem((lines, 128), jnp.int32),
        vmem((nx * rows, 128), F32), vmem((nx * rows, 128), F32), vmem((nx * rows, 128), F32),
        vmem((nx, lines, 128), F32), vmem((nx - 1, lines, 128), F32), vmem((lines, 128), F32),
        vmem((8, lines, 128), F32), vmem((2, 1, 128), F32), vmem((nf, 1, 128), F32), vmem((ns, 1, 128), F32),
        dma((6,)), dma((nx - 1,)), dma((nx - 1,)), dma((nx - 1,)), dma((nx - 1,)), dma((nx - 1,)), dma((nx - 1,)),
        dma((2, half, nx)), dma((2, half, nx)), dma((2, 8)), dma((2, 8)), dma((nx - 1,)), dma((nx - 1,)),
        dma((8,)), dma((8,)), dma((2,)), dma((2,)),
    ]
    wide_out = jax.ShapeDtypeStruct(wide, F32)
    out = jax.ShapeDtypeStruct((cx, cy, cz), F32)
    whole = pl.BlockSpec(memory_space=vmem)
    operands = (x0, c, b, j, owner.reshape(lines, 128), slot.reshape(lines, 128))
    state = pl.pallas_call(
        functools.partial(body, nx, ny, nz),
        out_shape=(wide_out,) * 5 + (out, jax.ShapeDtypeStruct((8, 128), F32)),
        in_specs=[pl.BlockSpec(memory_space=pltpu.HBM)] * 6,
        out_specs=(whole,) * 7,
        scratch_shapes=scratch,
        compiler_params=pltpu.CompilerParams(collective_id=0, has_side_effects=True, vmem_limit_bytes=44 * 2**20),
        name="coupling_step",
    )(*[pltpu.with_memory_space_constraint(v, pltpu.HBM) for v in operands])
    chunk = pl.BlockSpec((8, cy, cz), lambda i: (i, 0, 0))
    return pl.pallas_call(
        finish,
        grid=(cx // 8,),
        out_shape=(out, out),
        in_specs=[whole] * 7,
        out_specs=(chunk, chunk),
        compiler_params=pltpu.CompilerParams(vmem_limit_bytes=16 * 2**20),
        name="finish_step",
    )(*state)


def solution(mesh):
    nx, nz = XCHIPS, mesh.shape["solid"] // CORES
    ny = mesh.shape["fluid"] // nx
    both = ("fluid", "solid")
    block = P("fluid", "solid", None)
    return jax.shard_map(
        functools.partial(per_device, nx, ny, nz),
        mesh=mesh,
        in_specs=(block, block, P(None, both), P(None, both), P(both, None), P(both)),
        out_specs=(block, block),
        check_vma=False,
    )
```

```python
import functools

import jax
import jax.numpy as jnp
from jax import lax
from jax.experimental import pallas as pl
from jax.experimental.pallas import tpu as pltpu
from jax.sharding import PartitionSpec as P

ITERS = 3
XCHIPS = 4
CORES = 2
MESH = pl.DeviceIdType.MESH
F32 = jnp.float32
BF16 = jnp.bfloat16
AROUND = [(a, b) for a in (-1, 0, 1) for b in (-1, 0, 1) if (a, b) != (0, 0)]
LOW = 5
SIDE = 8


def iota(shape, axis):
    return lax.broadcasted_iota(jnp.int32, shape, axis)


def body(
    nx, ny, nz,
    x0_hbm, c_hbm, b_hbm, j_hbm, owner_hbm, slot_hbm,
    field, w0, w1, w2, last, coefs,
    bv, jv, idx, tabs, held, jac, codes, code_own, key, jm, acc,
    part_out, part_in, cross_in, edge, sum_out, sum_plane, sum_line,
    load_sem, bx_send, bx_recv, jx_send, jx_recv, cx_send, cx_recv,
    ring_send, ring_recv, halo_send, halo_recv, row_send, row_recv, cross_send, cross_recv, ar_send, ar_recv,
):
    xe, de = field.at[0], field.at[1]
    cx, cy, cz = (xe.shape[0] - 10, xe.shape[1] - 16, xe.shape[2])
    quads, faces = bv.shape
    rows = jv.shape[1]
    share = quads // nx
    many = 128 // share
    deep = faces // many
    rowsets = rows // 128
    f, s = lax.axis_index("fluid"), lax.axis_index("solid")
    nf, ns = nx * ny, nz * CORES
    x, y = lax.rem(f, nx), f // nx

    def remote(src, dst, send, recv, at):
        return pltpu.make_async_remote_copy(
            src_ref=src, dst_ref=dst, send_sem=send, recv_sem=recv,
            device_id=at, device_id_type=MESH,
        )

    def beside(a, b):
        return (lax.rem(f + a + nf, nf), lax.rem(s + b + ns, ns))

    def on_x(d):
        return (y * nx + lax.rem(x + d, nx), s)

    def on_y(d):
        return (lax.rem(y + d, ny) * nx + x, s)

    def in_row(a, d, b):
        return (lax.rem(y + a + ny, ny) * nx + lax.rem(x + d, nx), lax.rem(s + b + ns, ns))

    def on_plane(n):
        return (lax.rem(f + n, nf), s)

    def on_line(n):
        return (f, lax.rem(s + n, ns))

    inner = (pl.ds(LOW, cx), pl.ds(SIDE, cy))
    loads = [
        pltpu.make_async_copy(b_hbm, bv, load_sem.at[0]),
        pltpu.make_async_copy(owner_hbm, idx.at[0], load_sem.at[1]),
        pltpu.make_async_copy(slot_hbm, idx.at[1], load_sem.at[2]),
        pltpu.make_async_copy(j_hbm, jv, load_sem.at[3]),
        pltpu.make_async_copy(x0_hbm, xe.at[inner], load_sem.at[4]),
        pltpu.make_async_copy(c_hbm, de.at[inner], load_sem.at[5]),
    ]
    for load in loads:
        load.start()

    barrier = pltpu.get_barrier_semaphore()
    partners = [on_x(d) for d in range(1, nx)] + [on_line(n) for n in range(1, ns)]
    partners += [in_row(0, d, b) for d in range(1, nx) for b in (-1, 1)]
    partners += [on_y(1), on_y(ny - 1)] + [beside(a, b) for a, b in AROUND if a != 0]
    for at in partners:
        pl.semaphore_signal(barrier, inc=1, device_id=at, device_id_type=MESH)

    @pl.when(x == 0)
    def _():
        for b in (-1, 0, 1):
            for d in range(nx):
                pl.semaphore_signal(barrier, inc=1, device_id=in_row(-1, d, b), device_id_type=MESH)

    @pl.when(x == nx - 1)
    def _():
        for b in (-1, 0, 1):
            for d in range(nx):
                pl.semaphore_signal(barrier, inc=1, device_id=in_row(1, d, b), device_id_type=MESH)

    guard = jnp.zeros(xe.shape[1:], F32)
    for ref in (xe, w0, w1, w2):
        ref[0] = guard
        ref[cx + 9] = guard

    with jax.named_scope("tables"):
        loads[0].wait()
        for a in range(nx):
            mine = bv[a * share : (a + 1) * share, :]
            stack = jnp.concatenate(
                [mine[:, (m * deep // 128) * 128 : (m * deep // 128) * 128 + 128] for m in range(many)], axis=0
            )
            if deep < 128:
                turned = pltpu.roll(stack, 128 - deep, 1)
                odd = (iota(stack.shape, 0) // share) % 2 == 1
                stack = jnp.where(odd, turned, stack)
            tabs[a] = stack.T[:deep]
        loads[1].wait()
        loads[2].wait()
        code_own[...] = idx[0] * faces + idx[1]
        codes[0] = code_own[...]
        held[y, 0] = tabs[x]
        loads[3].wait()
        jac[0] = jv[pl.ds(pl.multiple_of(x * share, share), share), :]
        loads[4].wait()
        loads[5].wait()

    with jax.named_scope("entry"):
        pl.semaphore_wait(barrier, len(partners) + 6)

    spread = []
    for d in range(1, nx):
        remote(code_own, codes.at[d], cx_send, cx_recv, on_x(d)).start()
    some = pl.ds(0, nx - 1)
    coded = remote(codes.at[some], codes.at[some], cx_send, cx_recv, on_x(1))
    jacs = remote(jac.at[some], jac.at[some], jx_send, jx_recv, on_x(1))
    spread_all = remote(tabs.at[some], tabs.at[some], bx_send, bx_recv.at[0], on_x(1))
    ring_all = remote(held.at[pl.ds(0, ny - 1)], held.at[pl.ds(0, ny - 1)], ring_send, bx_recv.at[0], on_x(1))
    for d in range(1, nx):
        to = lax.rem(x + d, nx)
        spread.append(remote(tabs.at[to], held.at[y, d], bx_send, bx_recv.at[d - 1], on_x(d)))
        spread[-1].start()

    def ring(t, d, way):
        slot = lax.rem(y + ny + (1 - t if way == 0 else t - 1), ny)
        at = on_y(1 if way == 0 else ny - 1)
        block = held.at[slot, d]
        return remote(block, block, ring_send, ring_recv.at[way, t - 1, d], at)

    half = ny // 2

    def goes(t, d, way):
        return t < half or (d < nx // 2) == (way == 0)

    ways = [
        [[ring(t, d, way) if goes(t, d, way) else None for way in range(2)] for d in range(nx)]
        for t in range(1, half + 1)
    ]

    def forward(t, d):
        if t == 1 and d > 0:
            spread[d - 1].wait_recv()
        for way in range(2):
            if t > 1:
                ways[t - 2][d][way].wait_recv()
            if goes(t, d, way):
                ways[t - 1][d][way].start()

    forward(1, 0)
    def prepare_keys(d):
        for i in range(rowsets):
            code = codes[d, i : i + 1, :]
            owner, slot = code // faces, lax.rem(code, faces)
            keys = (owner * deep + lax.rem(slot, deep)).astype(F32)
            key[d * rows + i * 128 : d * rows + (i + 1) * 128, :] = jnp.broadcast_to(keys, (128, 128)).T

    def prepare_jac(d):
        for i in range(rowsets):
            slot = lax.rem(codes[d, i : i + 1, :], faces)
            j = jac[d, :, i * 128 : (i + 1) * 128]
            tiled = jnp.concatenate([j] * many, axis=0)
            wanted = iota((128, 128), 0) // share == jnp.broadcast_to(slot // deep, (128, 128))
            jm[d * rows + i * 128 : d * rows + (i + 1) * 128, :] = jnp.where(wanted, tiled, 0.0).T

    def weight(slot):
        parts = []
        for d in range(nx):
            parts.append(held[slot, d])
        table = jnp.concatenate(parts, axis=0)
        high = table.astype(BF16)
        low = (table - high.astype(F32)).astype(BF16)
        return jnp.concatenate([high, low], axis=1)

    def base_of(slot, d):
        return (slot * nx + lax.rem(x - d + nx, nx)) * deep

    tall = 512

    def pick(d, slots, first=False, finish=False):
        table = jnp.concatenate([weight(slot) for slot in slots], axis=0)
        lanes = iota((1, 128), 1)
        marks = []
        for slot in slots:
            for tile in range(nx * deep // 128):
                mark = jnp.zeros((1, 128), jnp.int32)
                for e in range(128 // deep):
                    p = tile * (128 // deep) + e
                    mark = jnp.where(lanes // deep == e, base_of(slot, p) + lanes - e * deep, mark)
                marks.append(mark.astype(F32))
        for i in range(rows // tall):
            place = pl.ds(d * rows + i * tall, tall)
            keys = key[place, :]
            hot = jnp.concatenate([jnp.where(keys == mark, 1.0, 0.0).astype(BF16) for mark in marks], axis=1)
            both = jnp.dot(hot, table, preferred_element_type=F32)
            got = both[:, :128] + both[:, 128:]
            if not first:
                got = got + acc[place, :]
            if not finish:
                acc[place, :] = got
                continue
            product = got * jm[place, :]
            for k in range(tall // 128):
                line = jnp.sum(product[k * 128 : (k + 1) * 128].T, axis=0, keepdims=True)
                at = i * (tall // 128) + k
                part_out[lax.rem(x - d + nx, nx), pl.ds(at, 1), :] = line

    def around_sum(ref, r, n):
        mid = ref[pl.ds(r, n)].reshape(n * xe.shape[1], cz)
        out = ref[pl.ds(r - 1, n)] + ref[pl.ds(r + 1, n)]
        out = out.reshape(n * xe.shape[1], cz)
        out = out + (pltpu.roll(mid, 1, 0) + pltpu.roll(mid, mid.shape[0] - 1, 0))
        lane = iota(mid.shape, 1)
        out = out + jnp.where(lane == 0, 0.0, pltpu.roll(mid, 1, 1))
        out = out + jnp.where(lane == cz - 1, 0.0, pltpu.roll(mid, cz - 1, 1))
        return out.reshape(n, xe.shape[1], cz)

    def start_solid():
        for ref, fill in ((xe, 0.0), (de, 1e30)):
            @pl.when(f == 0)
            def _():
                ref[pl.ds(LOW - 4, 4)] = jnp.full((4,) + xe.shape[1:], fill, F32)

            @pl.when(f == nf - 1)
            def _():
                ref[pl.ds(LOW + cx, 4)] = jnp.full((4,) + xe.shape[1:], fill, F32)

            @pl.when(s == 0)
            def _():
                ref[pl.ds(1, cx + 8), pl.ds(0, 8)] = jnp.full((cx + 8, 8, cz), fill, F32)

            @pl.when(s == ns - 1)
            def _():
                ref[pl.ds(1, cx + 8), pl.ds(SIDE + cy, 8)] = jnp.full((cx + 8, 8, cz), fill, F32)

        def one(i, carry):
            r = 1 + 8 * i
            got = around_sum(xe, r, 8) - 6.0 * xe[pl.ds(r, 8)]
            c = de[pl.ds(r, 8)]
            inverse = jnp.where(c > 1e29, 0.0, 1.0 / (6.0 + c))
            de[pl.ds(r, 8)] = inverse
            w0[pl.ds(r, 8)] = inverse * got
            return carry

        lax.fori_loop(0, (cx + 8) // 8, one, 0)

    order = sorted(range(nx), key=lambda d: (min(d, nx - d), -d))
    for d in order:
        if d == order[1]:
            coded.wait_recv()
        if d > 0:
            with jax.named_scope(f"forward#t=1#d={d}"):
                forward(1, d)
        with jax.named_scope(f"prepare_keys#d={d}"):
            prepare_keys(d)

    for d in range(1, nx):
        to = lax.rem(x + d, nx)
        remote(
            jv.at[pl.ds(pl.multiple_of(to * share, share), share)], jac.at[d], jx_send, jx_recv, on_x(d)
        ).start()
    to_x = {-1: (pl.ds(LOW, 4), pl.ds(LOW + cx, 4)), 0: (pl.ds(LOW, cx),) * 2, 1: (pl.ds(LOW + cx - 4, 4), pl.ds(LOW - 4, 4))}
    to_y = {-1: (pl.ds(SIDE, 8), pl.ds(SIDE + cy, 8)), 0: (pl.ds(SIDE, cy),) * 2, 1: (pl.ds(SIDE + cy - 8, 8), pl.ds(SIDE - 8, 8))}
    def group(a, b):
        return 0 if a == 0 else 1 if b == 0 else 2

    def send_halos(groups):
        for a, b in AROUND:
            k = group(a, b)
            if k in groups:
                remote(
                    field.at[:, to_x[a][0], to_y[b][0]], field.at[:, to_x[a][1], to_y[b][1]],
                    halo_send.at[k], halo_recv.at[k], beside(a, b),
                ).start()

    rims = [
        field.at[:, pl.ds(LOW, cx), pl.ds(0, 16)],
        field.at[:, pl.ds(LOW - 4, 8), pl.ds(SIDE, cy)],
        field.at[:, pl.ds(LOW - 4, 8), pl.ds(0, 16)],
    ]
    halos = [remote(rim, rim, halo_send.at[k], halo_recv.at[k], on_x(1)) for k, rim in enumerate(rims)]
    send_halos((0,))

    def near(far):
        if far == 0:
            return [y]
        return [lax.rem(y + ny - far, ny), lax.rem(y + far, ny)]

    for t in range(2, half + 1):
        for d in order:
            with jax.named_scope(f"forward#t={t}#d={d}"):
                forward(t, d)
            with jax.named_scope(f"pick#t={t}#d={d}"):
                pick(d, near(t - 2), first=t == 2)
            if t == half:
                if d == 0:
                    jacs.wait_recv()
                with jax.named_scope(f"prepare_jac#d={d}"):
                    prepare_jac(d)
    send_halos((1, 2))
    if half == 1:
        jacs.wait_recv()
        for d in range(nx):
            prepare_jac(d)
    for d in range(nx):
        with jax.named_scope(f"pick_near#d={d}"):
            pick(d, near(half - 1), first=half == 1)
    with jax.named_scope("far_wait"):
        for d in range(nx):
            for way in range(2):
                if goes(half, d, way):
                    ways[half - 1][d][way].wait_recv()
    for d in range(nx):
        with jax.named_scope(f"pick_far#d={d}"):
            pick(d, [lax.rem(y + half, ny)], finish=True)

    part_in[nx + x] = part_out[...]
    for b in (-1, 0, 1):
        slot = (1 - b) * nx + x
        remote(part_out.at[nx - 1], cross_in.at[0, slot], cross_send, cross_recv.at[0], in_row(1, nx - x, b)).start()
        remote(part_out.at[0], cross_in.at[1, slot], cross_send, cross_recv.at[1], in_row(-1, 2 * nx - 1 - x, b)).start()
        for d in range(nx):
            if (d, b) != (0, 0):
                remote(part_out, part_in.at[slot], row_send, row_recv, in_row(0, d, b)).start()
    most = part_in.at[pl.ds(0, 3 * nx - 1)]
    rows_all = remote(most, most, row_send, row_recv, on_x(1))
    six = cross_in.at[0, pl.ds(0, 6)]
    cross_all = remote(six, six, cross_send, cross_recv.at[0], on_x(1))
    with jax.named_scope("solid_wait"):
        for halo in halos:
            halo.wait_send()
        for halo in halos:
            halo.wait_recv()
    with jax.named_scope("solid_start"):
        start_solid()
    with jax.named_scope("part_wait"):
        rows_all.wait_recv()
        for side, end in ((0, 0), (1, nx - 1)):
            @pl.when(x == end)
            def _():
                whole = cross_in.at[side]
                remote(whole, whole, cross_send, cross_recv.at[side], on_x(1)).wait_recv()

    per = 128 // cy

    def heat(r, first, count, line, offset):
        shape = (per, count, 128)
        spot = iota(shape, 2)
        picked = jnp.where(spot == iota(shape, 0) * cy + iota(shape, 1) + offset, line.reshape(1, 1, 128), 0.0)
        column = jnp.sum(picked, axis=2, keepdims=True)
        here = (pl.ds(r, per), pl.ds(first, count))
        w0[here] = w0[here] + jnp.where(spot == cz - 1, column * de[here], 0.0)

    def gathered(b, reader, spots):
        return sum(part_in[(b + 1) * nx + h, reader, spots, :] for h in range(nx))

    with jax.named_scope("heat"):
        for a, end, side, spot in ((1, nx - 1, 1, 0), (-1, 0, 0, cx // per - 1)):
            for b in (-1, 0, 1):
                here = pl.ds(3 * side + b + 1, 1)

                @pl.when(x == end)
                def _():
                    edge[here, :] = sum(cross_in[side, (b + 1) * nx + h, spot : spot + 1, :] for h in range(nx))

                @pl.when(x != end)
                def _():
                    edge[here, :] = gathered(b, lax.rem(x + a + nx, nx), slice(spot, spot + 1))

        for a in (-1, 0, 1):
            for b in (-1, 0, 1):
                first = {0: SIDE, -1: 0, 1: SIDE + cy}[b]
                count = {0: cy, -1: 8, 1: 8}[b]
                offset = {0: 0, -1: cy - 8, 1: 0}[b]
                if a == 0:
                    block = gathered(b, x, slice(0, cx // per))
                    for i in range(cx // per):
                        heat(LOW + i * per, first, count, block[i : i + 1], offset)
                else:
                    at = 3 * (1 if a == 1 else 0) + b + 1
                    heat(LOW + cx if a == 1 else LOW - 4, first, count, edge[at : at + 1, :], offset)

    def fold(v):
        return jnp.sum(v.reshape(-1, 8, cz), axis=0)

    def inside(v):
        return v[:, SIDE : SIDE + cy]

    def step(ref, new, first):
        def one(i, carry):
            r = LOW + 8 * i
            near = around_sum(ref, r, 8)
            inverse = de[pl.ds(r, 8)]
            new_w = inverse * near
            new[pl.ds(r, 8)] = new_w
            now = inside(ref[pl.ds(r, 8)])
            near = inside(near)
            odd = carry[0] + fold(now * near)
            even = carry[1] + fold(inside(new_w) * near)
            if first:
                return (odd, even, carry[2] + fold(now * now / inside(inverse)))
            return (odd, even)

        zero = jnp.zeros((8, cz), F32)
        sums = lax.fori_loop(0, cx // 8, one, (zero,) * (3 if first else 2))
        for r in (LOW - 4, LOW + cx):
            new[pl.ds(r, 4)] = de[pl.ds(r, 4)] * around_sum(ref, r, 4)
        return sums

    with jax.named_scope("step#k=0"):
        mu1, mu2, mu0 = step(w0, w1, True)
    with jax.named_scope("step#k=1"):
        mu3, mu4 = step(w1, w2, False)

    def final(i, carry):
        near = inside(around_sum(w2, LOW + 8 * i, 8))
        last[pl.ds(8 * i, 8)] = near
        return carry + fold(inside(w2[pl.ds(LOW + 8 * i, 8)]) * near)

    with jax.named_scope("step#k=2"):
        mu5 = lax.fori_loop(0, cx // 8, final, jnp.zeros((8, cz), F32))
    lines = [jnp.sum(v, axis=0, keepdims=True) for v in (mu0, mu1, mu2, mu3, mu4, mu5)]
    lines.append(jnp.zeros((2, cz), F32))
    sums = jnp.sum(jnp.concatenate(lines, axis=0), axis=1, keepdims=True)
    local = jnp.sum(jnp.where(iota((8, 128), 0) == iota((8, 128), 1), sums, 0.0), axis=0, keepdims=True)
    sends = []

    def reduce(stage, value, slots, me, peers):
        sum_out[stage] = value
        slots[me] = value
        for at in peers:
            remote(sum_out.at[stage], slots.at[me], ar_send.at[stage], ar_recv.at[stage], at).start()
        every = slots.at[pl.ds(0, len(peers))]
        everyone = remote(every, every, ar_send.at[stage], ar_recv.at[stage], peers[0])
        everyone.wait_recv()
        sends.append(everyone)
        return jnp.sum(slots[...], axis=0)

    with jax.named_scope("reduce#k=0"):
        local = reduce(0, local, sum_plane, f, [on_plane(n) for n in range(1, nf)])
    with jax.named_scope("reduce#k=1"):
        local = reduce(1, local, sum_line, s, [on_line(n) for n in range(1, ns)])
    lane = iota((1, 128), 1)
    mu = [jnp.sum(jnp.where(lane == k, local, 0.0), axis=1, keepdims=True) for k in range(6)]
    mu = [jnp.broadcast_to(m, (1, 128)) for m in mu]

    def product(u, v):
        out = 0.0
        for a, left in enumerate(u):
            for b, right in enumerate(v):
                out = out + left * right * mu[a + b]
        return out

    one_line = jnp.ones((1, cz), F32)
    course, misfit, guess = [one_line], [one_line], []
    rz = mu[0]
    for it in range(ITERS):
        image = [
            (course[k] if k < len(course) else 0.0) - (course[k - 1] if k > 0 else 0.0)
            for k in range(len(course) + 1)
        ]
        alpha = rz / product(course, image)
        guess = [(guess[k] if k < len(guess) else 0.0) + alpha * course[k] for k in range(len(course))]
        misfit = [(misfit[k] if k < len(misfit) else 0.0) - alpha * image[k] for k in range(len(image))]
        if it + 1 < ITERS:
            new = product(misfit, misfit)
            ratio = new / rz
            course = [misfit[k] + (ratio * course[k] if k < len(course) else 0.0) for k in range(len(misfit))]
            rz = new

    coefs[...] = jnp.concatenate(guess + misfit + [one_line], axis=0)
    with jax.named_scope("sent"):
        for copy in [spread_all, coded, jacs, ring_all, rows_all, cross_all] + sends:
            copy.wait_send()


def finish(field, w0, w1, w2, last, coefs, guess, misfit):
    xe, de = field.at[0], field.at[1]
    n, cy, _ = guess.shape
    first = pl.program_id(0) * n
    here = (pl.ds(LOW + first, n), pl.ds(SIDE, cy))
    line = [coefs[k : k + 1, :] for k in range(7)]
    basis = [w0[here], w1[here], w2[here]]
    guess[...] = xe[here] + (line[0] * basis[0] + (line[1] * basis[1] + line[2] * basis[2]))
    rest = line[3] * basis[0] + (line[4] * basis[1] + line[5] * basis[2])
    misfit[...] = rest / de[here] + line[6] * last[pl.ds(first, n)]


def per_device(nx, ny, nz, x0, c, b, j, owner, slot):
    quads, faces = b.shape
    rows = slot.shape[0]
    cx, cy, cz = x0.shape
    share = quads // nx
    deep = faces * share // 128
    half = ny // 2
    wide = (cx + 10, cy + 16, cz)
    lines = rows // 128
    nf, ns = nx * ny, nz * CORES
    dma = pltpu.SemaphoreType.DMA
    vmem = pltpu.VMEM
    scratch = [
        vmem((quads, faces), F32), vmem((quads, rows), F32), vmem((2, lines, 128), jnp.int32),
        vmem((nx, deep, 128), F32), vmem((ny, nx, deep, 128), F32), vmem((nx, share, rows), F32),
        vmem((nx, lines, 128), jnp.int32), vmem((lines, 128), jnp.int32),
        vmem((nx * rows, 128), F32), vmem((nx * rows, 128), F32), vmem((nx * rows, 128), F32),
        vmem((nx, lines, 128), F32), vmem((3 * nx, nx, lines, 128), F32), vmem((2, 3 * nx, lines, 128), F32), vmem((8, 128), F32),
        vmem((2, 1, 128), F32), vmem((nf, 1, 128), F32), vmem((ns, 1, 128), F32),
        dma((6,)), dma, dma((nx - 1,)), dma, dma, dma, dma,
        dma, dma((2, half, nx)), dma((3,)), dma((3,)), dma, dma, dma, dma((2,)), dma((2,)), dma((2,)),
    ]
    wide_out = jax.ShapeDtypeStruct(wide, F32)
    out = jax.ShapeDtypeStruct((cx, cy, cz), F32)
    whole = pl.BlockSpec(memory_space=vmem)
    operands = (x0, c, b, j, owner.reshape(lines, 128), slot.reshape(lines, 128))
    state = pl.pallas_call(
        functools.partial(body, nx, ny, nz),
        out_shape=(jax.ShapeDtypeStruct((2,) + wide, F32),) + (wide_out,) * 3 + (out, jax.ShapeDtypeStruct((8, 128), F32)),
        in_specs=[pl.BlockSpec(memory_space=pltpu.HBM)] * 6,
        out_specs=(whole,) * 6,
        scratch_shapes=scratch,
        compiler_params=pltpu.CompilerParams(collective_id=0, has_side_effects=True, vmem_limit_bytes=44 * 2**20),
        name="coupling_step",
    )(*[pltpu.with_memory_space_constraint(v, pltpu.HBM) for v in operands])
    chunk = pl.BlockSpec((8, cy, cz), lambda i: (i, 0, 0))
    return pl.pallas_call(
        finish,
        grid=(cx // 8,),
        out_shape=(out, out),
        in_specs=[whole] * 6,
        out_specs=(chunk, chunk),
        compiler_params=pltpu.CompilerParams(vmem_limit_bytes=16 * 2**20),
        name="finish_step",
    )(*state)


def solution(mesh):
    nx, nz = XCHIPS, mesh.shape["solid"] // CORES
    ny = mesh.shape["fluid"] // nx
    both = ("fluid", "solid")
    block = P("fluid", "solid", None)
    return jax.shard_map(
        functools.partial(per_device, nx, ny, nz),
        mesh=mesh,
        in_specs=(block, block, P(None, both), P(None, both), P(both, None), P(both)),
        out_specs=(block, block),
        check_vma=False,
    )
```

```python
import functools

import jax
import jax.numpy as jnp
from jax import lax
from jax.experimental import pallas as pl
from jax.experimental.pallas import tpu as pltpu
from jax.sharding import PartitionSpec as P

ITERS = 3
XCHIPS = 4
CORES = 2
MESH = pl.DeviceIdType.MESH
F32 = jnp.float32
BF16 = jnp.bfloat16
AROUND = [(a, b) for a in (-1, 0, 1) for b in (-1, 0, 1) if (a, b) != (0, 0)]
LOW = 5
SIDE = 8


def iota(shape, axis):
    return lax.broadcasted_iota(jnp.int32, shape, axis)


def body(
    nx, ny, nz,
    x0_hbm, c_hbm, b_hbm, j_hbm, owner_hbm, slot_hbm,
    field, w0, w1, w2, last, coefs,
    bv, jv, idx, tabs, held, jac, codes, code_own, key, jm, acc,
    part_out, part_in, cross_in, edge, sum_out, sum_plane, sum_line,
    load_sem, bx_send, bx_recv, jx_send, jx_recv, cx_send, cx_recv,
    ring_send, ring_recv, halo_send, halo_recv, row_send, row_recv, cross_send, cross_recv, ar_send, ar_recv, tokens,
):
    xe, de = field.at[0], field.at[1]
    cx, cy, cz = (xe.shape[0] - 10, xe.shape[1] - 16, xe.shape[2])
    quads, faces = bv.shape
    rows = jv.shape[1]
    share = quads // nx
    many = 128 // share
    deep = faces // many
    rowsets = rows // 128
    f, s = lax.axis_index("fluid"), lax.axis_index("solid")
    nf, ns = nx * ny, nz * CORES
    x, y = lax.rem(f, nx), f // nx

    def remote(src, dst, send, recv, at):
        return pltpu.make_async_remote_copy(
            src_ref=src, dst_ref=dst, send_sem=send, recv_sem=recv,
            device_id=at, device_id_type=MESH,
        )

    def beside(a, b):
        return (lax.rem(f + a + nf, nf), lax.rem(s + b + ns, ns))

    def on_x(d):
        return (y * nx + lax.rem(x + d, nx), s)

    def on_y(d):
        return (lax.rem(y + d, ny) * nx + x, s)

    def in_row(a, d, b):
        return (lax.rem(y + a + ny, ny) * nx + lax.rem(x + d, nx), lax.rem(s + b + ns, ns))

    def on_plane(n):
        return (lax.rem(f + n, nf), s)

    def on_line(n):
        return (f, lax.rem(s + n, ns))

    inner = (pl.ds(LOW, cx), pl.ds(SIDE, cy))
    loads = [
        pltpu.make_async_copy(b_hbm, bv, load_sem.at[0]),
        pltpu.make_async_copy(owner_hbm, idx.at[0], load_sem.at[1]),
        pltpu.make_async_copy(slot_hbm, idx.at[1], load_sem.at[2]),
        pltpu.make_async_copy(j_hbm, jv, load_sem.at[3]),
        pltpu.make_async_copy(x0_hbm, xe.at[inner], load_sem.at[4]),
        pltpu.make_async_copy(c_hbm, de.at[inner], load_sem.at[5]),
    ]
    for load in loads:
        load.start()

    barrier = pltpu.get_barrier_semaphore()
    partners = [on_x(d) for d in range(1, nx)] + [on_y(1), on_y(ny - 1), beside(0, -1), beside(0, 1)]
    for at in partners:
        pl.semaphore_signal(barrier, inc=1, device_id=at, device_id_type=MESH)

    def tell(kind, low, high):
        pl.semaphore_signal(tokens.at[kind, 0], inc=1, device_id=low, device_id_type=MESH)
        pl.semaphore_signal(tokens.at[kind, 1], inc=1, device_id=high, device_id_type=MESH)

    def hear(kind):
        pl.semaphore_wait(tokens.at[kind, 0], 1)
        pl.semaphore_wait(tokens.at[kind, 1], 1)

    guard = jnp.zeros(xe.shape[1:], F32)
    for ref in (xe, w0, w1, w2):
        ref[0] = guard
        ref[cx + 9] = guard

    for end in (0, nx * rowsets + 1):
        part_out[end] = jnp.zeros((1, 128), F32)

    with jax.named_scope("tables"):
        loads[0].wait()
        for a in range(nx):
            mine = bv[a * share : (a + 1) * share, :]
            stack = jnp.concatenate(
                [mine[:, (m * deep // 128) * 128 : (m * deep // 128) * 128 + 128] for m in range(many)], axis=0
            )
            if deep < 128:
                turned = pltpu.roll(stack, 128 - deep, 1)
                odd = (iota(stack.shape, 0) // share) % 2 == 1
                stack = jnp.where(odd, turned, stack)
            tabs[a] = stack.T[:deep]
        loads[1].wait()
        loads[2].wait()
        code_own[...] = idx[0] * faces + idx[1]
        codes[0] = code_own[...]
        held[y, 0] = tabs[x]
        loads[3].wait()
        jac[0] = jv[pl.ds(pl.multiple_of(x * share, share), share), :]
        loads[4].wait()
        loads[5].wait()

    with jax.named_scope("entry"):
        pl.semaphore_wait(barrier, len(partners))
        tell(0, beside(0, -1), beside(0, 1))

    spread = []
    for d in range(1, nx):
        remote(code_own, codes.at[d], cx_send, cx_recv, on_x(d)).start()
    some = pl.ds(0, nx - 1)
    coded = remote(codes.at[some], codes.at[some], cx_send, cx_recv, on_x(1))
    jacs = remote(jac.at[some], jac.at[some], jx_send, jx_recv, on_x(1))
    spread_all = remote(tabs.at[some], tabs.at[some], bx_send, bx_recv.at[0], on_x(1))
    ring_all = remote(held.at[pl.ds(0, ny - 1)], held.at[pl.ds(0, ny - 1)], ring_send, bx_recv.at[0], on_x(1))
    for d in range(1, nx):
        to = lax.rem(x + d, nx)
        spread.append(remote(tabs.at[to], held.at[y, d], bx_send, bx_recv.at[d - 1], on_x(d)))
        spread[-1].start()

    def ring(t, d, way):
        slot = lax.rem(y + ny + (1 - t if way == 0 else t - 1), ny)
        at = on_y(1 if way == 0 else ny - 1)
        block = held.at[slot, d]
        return remote(block, block, ring_send, ring_recv.at[way, t - 1, d], at)

    half = ny // 2

    def goes(t, d, way):
        return t < half or (d < nx // 2) == (way == 0)

    ways = [
        [[ring(t, d, way) if goes(t, d, way) else None for way in range(2)] for d in range(nx)]
        for t in range(1, half + 1)
    ]

    def forward(t, d):
        if t == 1 and d > 0:
            spread[d - 1].wait_recv()
        for way in range(2):
            if t > 1:
                ways[t - 2][d][way].wait_recv()
            if goes(t, d, way):
                ways[t - 1][d][way].start()

    forward(1, 0)
    def prepare_keys(d):
        for i in range(rowsets):
            code = codes[d, i : i + 1, :]
            owner, slot = code // faces, lax.rem(code, faces)
            keys = (owner * deep + lax.rem(slot, deep)).astype(F32)
            key[d * rows + i * 128 : d * rows + (i + 1) * 128, :] = jnp.broadcast_to(keys, (128, 128)).T

    def prepare_jac(d):
        for i in range(rowsets):
            slot = lax.rem(codes[d, i : i + 1, :], faces)
            j = jac[d, :, i * 128 : (i + 1) * 128]
            tiled = jnp.concatenate([j] * many, axis=0)
            wanted = iota((128, 128), 0) // share == jnp.broadcast_to(slot // deep, (128, 128))
            jm[d * rows + i * 128 : d * rows + (i + 1) * 128, :] = jnp.where(wanted, tiled, 0.0).T

    def weight(slot):
        parts = []
        for d in range(nx):
            parts.append(held[slot, d])
        table = jnp.concatenate(parts, axis=0)
        high = table.astype(BF16)
        low = (table - high.astype(F32)).astype(BF16)
        return jnp.concatenate([high, low], axis=1)

    def base_of(slot, d):
        return (slot * nx + lax.rem(x - d + nx, nx)) * deep

    tall = 512

    def pick(d, slots, first=False, finish=False):
        table = jnp.concatenate([weight(slot) for slot in slots], axis=0)
        lanes = iota((1, 128), 1)
        marks = []
        for slot in slots:
            for tile in range(nx * deep // 128):
                mark = jnp.zeros((1, 128), jnp.int32)
                for e in range(128 // deep):
                    p = tile * (128 // deep) + e
                    mark = jnp.where(lanes // deep == e, base_of(slot, p) + lanes - e * deep, mark)
                marks.append(mark.astype(F32))
        for i in range(rows // tall):
            place = pl.ds(d * rows + i * tall, tall)
            keys = key[place, :]
            hot = jnp.concatenate([jnp.where(keys == mark, 1.0, 0.0).astype(BF16) for mark in marks], axis=1)
            both = jnp.dot(hot, table, preferred_element_type=F32)
            got = both[:, :128] + both[:, 128:]
            if not first:
                got = got + acc[place, :]
            if not finish:
                acc[place, :] = got
                continue
            product = got * jm[place, :]
            for k in range(tall // 128):
                line = jnp.sum(product[k * 128 : (k + 1) * 128].T, axis=0, keepdims=True)
                at = i * (tall // 128) + k
                part_out[1 + lax.rem(x - d + nx, nx) * rowsets + at] = line

    def around_sum(ref, r, n):
        mid = ref[pl.ds(r, n)].reshape(n * xe.shape[1], cz)
        out = ref[pl.ds(r - 1, n)] + ref[pl.ds(r + 1, n)]
        out = out.reshape(n * xe.shape[1], cz)
        out = out + (pltpu.roll(mid, 1, 0) + pltpu.roll(mid, mid.shape[0] - 1, 0))
        lane = iota(mid.shape, 1)
        out = out + jnp.where(lane == 0, 0.0, pltpu.roll(mid, 1, 1))
        out = out + jnp.where(lane == cz - 1, 0.0, pltpu.roll(mid, cz - 1, 1))
        return out.reshape(n, xe.shape[1], cz)

    def start_solid():
        for ref, fill in ((xe, 0.0), (de, 1e30)):
            @pl.when(f == 0)
            def _():
                ref[pl.ds(LOW - 4, 4)] = jnp.full((4,) + xe.shape[1:], fill, F32)

            @pl.when(f == nf - 1)
            def _():
                ref[pl.ds(LOW + cx, 4)] = jnp.full((4,) + xe.shape[1:], fill, F32)

            @pl.when(s == 0)
            def _():
                ref[pl.ds(1, cx + 8), pl.ds(0, 8)] = jnp.full((cx + 8, 8, cz), fill, F32)

            @pl.when(s == ns - 1)
            def _():
                ref[pl.ds(1, cx + 8), pl.ds(SIDE + cy, 8)] = jnp.full((cx + 8, 8, cz), fill, F32)

        def one(i, carry):
            r = 1 + 8 * i
            got = around_sum(xe, r, 8) - 6.0 * xe[pl.ds(r, 8)]
            c = de[pl.ds(r, 8)]
            inverse = jnp.where(c > 1e29, 0.0, 1.0 / (6.0 + c))
            de[pl.ds(r, 8)] = inverse
            w0[pl.ds(r, 8)] = inverse * got
            return carry

        lax.fori_loop(0, (cx + 8) // 8, one, 0)

    order = sorted(range(nx), key=lambda d: (min(d, nx - d), -d))

    def round_of(t):
        others = [(t, d) for d in order if d > 0]
        ahead = [(t + 2, 0)] if t + 2 <= half else []
        return ([(2, 0)] if t == 1 and half > 1 else []) + others + ahead

    prepare_keys(0)
    for n, (t, d) in enumerate(round_of(1)):
        with jax.named_scope(f"forward#t={t}#d={d}"):
            forward(t, d)
        if (t, d) == (1, order[1]):
            coded.wait_recv()
        if t == 1:
            prepare_keys(d)
    with jax.named_scope("hear#k=0"):
        hear(0)
    tell(1, on_y(ny - 1), on_y(1))
    if ns > 4:
        tell(2, beside(0, -2), beside(0, 2))
    for d in range(1, nx):
        to = lax.rem(x + d, nx)
        remote(
            jv.at[pl.ds(pl.multiple_of(to * share, share), share)], jac.at[d], jx_send, jx_recv, on_x(d)
        ).start()
    to_y = {-1: (pl.ds(SIDE, 8), pl.ds(SIDE + cy, 8)), 0: (pl.ds(SIDE, cy),) * 2, 1: (pl.ds(SIDE + cy - 8, 8), pl.ds(SIDE - 8, 8))}

    def send_side(a):
        def rows_of(count):
            if a == 1:
                return pl.ds(LOW + cx - count, count), pl.ds(LOW - count, count)
            return pl.ds(LOW, count), pl.ds(LOW + cx, count)

        near, near_to = rows_of(3)
        four, four_to = rows_of(4)
        fourth = pl.ds(LOW + cx - 4 if a == 1 else LOW + 3, 1)
        fourth_to = pl.ds(LOW - 4 if a == 1 else LOW + cx + 3, 1)
        sides = pl.ds(SIDE, cy)
        cuts = [
            (field.at[:, near, sides], field.at[:, near_to, sides], 1, 0),
            (field.at[0, fourth, sides], field.at[0, fourth_to, sides], 2, 0),
            (field.at[:, near, pl.ds(SIDE + cy - 4, 4)], field.at[:, near_to, pl.ds(SIDE - 4, 4)], 3, 1),
            (field.at[:, near, pl.ds(SIDE, 4)], field.at[:, near_to, pl.ds(SIDE + cy, 4)], 3, -1),
        ]
        for src, dst, k, b in cuts:
            remote(src, dst, halo_send.at[k], halo_recv.at[k], beside(a, b)).start()

    ends = ((1, nx - 1), (-1, 0))

    def send_sides(inside):
        for a, end in ends:
            @pl.when((x != end) if inside else (x == end))
            def _():
                send_side(a)

    for b in (-1, 1):
        remote(
            field.at[:, pl.ds(LOW, cx), to_y[b][0]], field.at[:, pl.ds(LOW, cx), to_y[b][1]],
            halo_send.at[0], halo_recv.at[0], beside(0, b),
        ).start()
    send_sides(True)
    rims = [
        field.at[:, pl.ds(LOW, cx), pl.ds(0, 16)],
        field.at[:, pl.ds(LOW - 3, 6), pl.ds(SIDE, cy)],
        field.at[0, pl.ds(LOW - 4, 2), pl.ds(SIDE, cy)],
        field.at[:, pl.ds(LOW - 3, 6), pl.ds(0, 8)],
    ]
    halos = [remote(rim, rim, halo_send.at[k], halo_recv.at[k], on_x(1)) for k, rim in enumerate(rims)]

    def near(far):
        if far == 0:
            return [y]
        return [lax.rem(y + ny - far, ny), lax.rem(y + far, ny)]

    def hear_more():
        hear(1)
        if ns > 4:
            hear(2)
        if ns > 8:
            tell(3, beside(0, -4), beside(0, 4))

    for t in range(2, half + 1):
        todo = round_of(t)
        for n, d in enumerate(order):
            if n < len(todo):
                with jax.named_scope(f"forward#t={t}#n={n}"):
                    forward(*todo[n])
            with jax.named_scope(f"pick#t={t}#d={d}"):
                pick(d, near(t - 2), first=t == 2)
            if t == max(2, half - 1):
                if d == 0:
                    hear_more()
                    jacs.wait_recv()
                with jax.named_scope(f"prepare_jac#d={d}"):
                    prepare_jac(d)
    send_sides(False)
    if half == 1:
        hear_more()
    if half == 1:
        jacs.wait_recv()
        for d in range(nx):
            prepare_jac(d)
    for d in range(nx):
        with jax.named_scope(f"pick_near#d={d}"):
            pick(d, near(half - 1), first=half == 1)
    if ns > 8:
        with jax.named_scope("hear#k=3"):
            hear(3)
    with jax.named_scope("far_wait"):
        for d in range(nx):
            for way in range(2):
                if goes(half, d, way):
                    ways[half - 1][d][way].wait_recv()
    for d in range(nx):
        with jax.named_scope(f"pick_far#d={d}"):
            pick(d, [lax.rem(y + half, ny)], finish=True)

    part_in[nx + x] = part_out[pl.ds(x * rowsets, rowsets + 2)]
    for b in (-1, 0, 1):
        slot = (1 - b) * nx + x
        for d in range(nx):
            if (d, b) != (0, 0):
                lines = part_out.at[pl.ds(lax.rem(x + d, nx) * rowsets, rowsets + 2)]
                remote(lines, part_in.at[slot], row_send, row_recv, in_row(0, d, b)).start()
        line = part_out.at[nx * rowsets]
        remote(line, cross_in.at[0, slot], cross_send, cross_recv.at[0], in_row(1, nx - x, b)).start()
        line = part_out.at[1]
        remote(line, cross_in.at[1, slot], cross_send, cross_recv.at[1], in_row(-1, 2 * nx - 1 - x, b)).start()
    most = part_in.at[pl.ds(0, 3 * nx - 1)]
    rows_all = remote(most, most, row_send, row_recv, on_x(1))
    six = cross_in.at[0, pl.ds(0, 6)]
    cross_all = remote(six, six, cross_send, cross_recv.at[0], on_x(1))
    with jax.named_scope("solid_wait"):
        for halo in halos:
            halo.wait_send()
        for halo in halos:
            halo.wait_recv()
    with jax.named_scope("solid_start"):
        start_solid()
    with jax.named_scope("part_wait"):
        rows_all.wait_recv()
        for side, end in ((0, 0), (1, nx - 1)):
            @pl.when(x == end)
            def _():
                whole = cross_in.at[side]
                remote(whole, whole, cross_send, cross_recv.at[side], on_x(1)).wait_recv()

    per = 128 // cy

    def heat(r, first, count, line, offset):
        shape = (per, count, 128)
        spot = iota(shape, 2)
        picked = jnp.where(spot == iota(shape, 0) * cy + iota(shape, 1) + offset, line.reshape(1, 1, 128), 0.0)
        column = jnp.sum(picked, axis=2, keepdims=True)
        here = (pl.ds(r, per), pl.ds(first, count))
        w0[here] = w0[here] + jnp.where(spot == cz - 1, column * de[here], 0.0)

    def gathered(b, spot):
        return sum(part_in[(b + 1) * nx + h, spot] for h in range(nx))

    with jax.named_scope("heat"):
        for a, end, side, spot in ((1, nx - 1, 1, rowsets + 1), (-1, 0, 0, 0)):
            for b in (-1, 0, 1):
                here = pl.ds(3 * side + b + 1, 1)

                @pl.when(x == end)
                def _():
                    edge[here, :] = sum(cross_in[side, (b + 1) * nx + h] for h in range(nx))

                @pl.when(x != end)
                def _():
                    edge[here, :] = gathered(b, spot)

        for a in (-1, 0, 1):
            for b in (-1, 0, 1):
                first = {0: SIDE, -1: 0, 1: SIDE + cy}[b]
                count = {0: cy, -1: 8, 1: 8}[b]
                offset = {0: 0, -1: cy - 8, 1: 0}[b]
                if a == 0:
                    for i in range(cx // per):
                        heat(LOW + i * per, first, count, gathered(b, 1 + i), offset)
                else:
                    at = 3 * (1 if a == 1 else 0) + b + 1
                    heat(LOW + cx if a == 1 else LOW - 4, first, count, edge[at : at + 1, :], offset)

    def fold(v):
        return jnp.sum(v.reshape(-1, 8, cz), axis=0)

    def inside(v):
        return v[:, SIDE : SIDE + cy]

    def step(ref, new, first):
        def one(i, carry):
            r = LOW + 8 * i
            near = around_sum(ref, r, 8)
            inverse = de[pl.ds(r, 8)]
            new_w = inverse * near
            new[pl.ds(r, 8)] = new_w
            now = inside(ref[pl.ds(r, 8)])
            near = inside(near)
            odd = carry[0] + fold(now * near)
            even = carry[1] + fold(inside(new_w) * near)
            if first:
                return (odd, even, carry[2] + fold(now * now / inside(inverse)))
            return (odd, even)

        zero = jnp.zeros((8, cz), F32)
        sums = lax.fori_loop(0, cx // 8, one, (zero,) * (3 if first else 2))
        for r in (LOW - 4, LOW + cx):
            new[pl.ds(r, 4)] = de[pl.ds(r, 4)] * around_sum(ref, r, 4)
        return sums

    with jax.named_scope("step#k=0"):
        mu1, mu2, mu0 = step(w0, w1, True)
    with jax.named_scope("step#k=1"):
        mu3, mu4 = step(w1, w2, False)

    def final(i, carry):
        near = inside(around_sum(w2, LOW + 8 * i, 8))
        last[pl.ds(8 * i, 8)] = near
        return carry + fold(inside(w2[pl.ds(LOW + 8 * i, 8)]) * near)

    with jax.named_scope("step#k=2"):
        mu5 = lax.fori_loop(0, cx // 8, final, jnp.zeros((8, cz), F32))
    lines = [jnp.sum(v, axis=0, keepdims=True) for v in (mu0, mu1, mu2, mu3, mu4, mu5)]
    lines.append(jnp.zeros((2, cz), F32))
    sums = jnp.sum(jnp.concatenate(lines, axis=0), axis=1, keepdims=True)
    local = jnp.sum(jnp.where(iota((8, 128), 0) == iota((8, 128), 1), sums, 0.0), axis=0, keepdims=True)
    sends = []

    def reduce(stage, value, slots, me, peers):
        sum_out[stage] = value
        slots[me] = value
        for at in peers:
            remote(sum_out.at[stage], slots.at[me], ar_send.at[stage], ar_recv.at[stage], at).start()
        every = slots.at[pl.ds(0, len(peers))]
        everyone = remote(every, every, ar_send.at[stage], ar_recv.at[stage], peers[0])
        everyone.wait_recv()
        sends.append(everyone)
        return jnp.sum(slots[...], axis=0)

    with jax.named_scope("reduce#k=0"):
        local = reduce(0, local, sum_plane, f, [on_plane(n) for n in range(1, nf)])
    with jax.named_scope("reduce#k=1"):
        local = reduce(1, local, sum_line, s, [on_line(n) for n in range(1, ns)])
    lane = iota((1, 128), 1)
    mu = [jnp.sum(jnp.where(lane == k, local, 0.0), axis=1, keepdims=True) for k in range(6)]
    mu = [jnp.broadcast_to(m, (1, 128)) for m in mu]

    def product(u, v):
        out = 0.0
        for a, left in enumerate(u):
            for b, right in enumerate(v):
                out = out + left * right * mu[a + b]
        return out

    one_line = jnp.ones((1, cz), F32)
    course, misfit, guess = [one_line], [one_line], []
    rz = mu[0]
    for it in range(ITERS):
        image = [
            (course[k] if k < len(course) else 0.0) - (course[k - 1] if k > 0 else 0.0)
            for k in range(len(course) + 1)
        ]
        alpha = rz / product(course, image)
        guess = [(guess[k] if k < len(guess) else 0.0) + alpha * course[k] for k in range(len(course))]
        misfit = [(misfit[k] if k < len(misfit) else 0.0) - alpha * image[k] for k in range(len(image))]
        if it + 1 < ITERS:
            new = product(misfit, misfit)
            ratio = new / rz
            course = [misfit[k] + (ratio * course[k] if k < len(course) else 0.0) for k in range(len(misfit))]
            rz = new

    coefs[...] = jnp.concatenate(guess + misfit + [one_line], axis=0)
    with jax.named_scope("sent"):
        for copy in [spread_all, coded, jacs, ring_all, rows_all, cross_all] + sends:
            copy.wait_send()


def finish(field, w0, w1, w2, last, coefs, guess, misfit):
    xe, de = field.at[0], field.at[1]
    n, cy, _ = guess.shape
    first = pl.program_id(0) * n
    here = (pl.ds(LOW + first, n), pl.ds(SIDE, cy))
    line = [coefs[k : k + 1, :] for k in range(7)]
    basis = [w0[here], w1[here], w2[here]]
    guess[...] = xe[here] + (line[0] * basis[0] + (line[1] * basis[1] + line[2] * basis[2]))
    rest = line[3] * basis[0] + (line[4] * basis[1] + line[5] * basis[2])
    misfit[...] = rest / de[here] + line[6] * last[pl.ds(first, n)]


def per_device(nx, ny, nz, x0, c, b, j, owner, slot):
    quads, faces = b.shape
    rows = slot.shape[0]
    cx, cy, cz = x0.shape
    share = quads // nx
    deep = faces * share // 128
    half = ny // 2
    wide = (cx + 10, cy + 16, cz)
    lines = rows // 128
    nf, ns = nx * ny, nz * CORES
    dma = pltpu.SemaphoreType.DMA
    vmem = pltpu.VMEM
    scratch = [
        vmem((quads, faces), F32), vmem((quads, rows), F32), vmem((2, lines, 128), jnp.int32),
        vmem((nx, deep, 128), F32), vmem((ny, nx, deep, 128), F32), vmem((nx, share, rows), F32),
        vmem((nx, lines, 128), jnp.int32), vmem((lines, 128), jnp.int32),
        vmem((nx * rows, 128), F32), vmem((nx * rows, 128), F32), vmem((nx * rows, 128), F32),
        vmem((nx * lines + 2, 1, 128), F32), vmem((3 * nx, lines + 2, 1, 128), F32), vmem((2, 3 * nx, 1, 128), F32), vmem((8, 128), F32),
        vmem((2, 1, 128), F32), vmem((nf, 1, 128), F32), vmem((ns, 1, 128), F32),
        dma((6,)), dma, dma((nx - 1,)), dma, dma, dma, dma,
        dma, dma((2, half, nx)), dma((4,)), dma((4,)), dma, dma, dma, dma((2,)), dma((2,)), dma((2,)),
        pltpu.SemaphoreType.REGULAR((4, 2)),
    ]
    wide_out = jax.ShapeDtypeStruct(wide, F32)
    out = jax.ShapeDtypeStruct((cx, cy, cz), F32)
    whole = pl.BlockSpec(memory_space=vmem)
    operands = (x0, c, b, j, owner.reshape(lines, 128), slot.reshape(lines, 128))
    state = pl.pallas_call(
        functools.partial(body, nx, ny, nz),
        out_shape=(jax.ShapeDtypeStruct((2,) + wide, F32),) + (wide_out,) * 3 + (out, jax.ShapeDtypeStruct((8, 128), F32)),
        in_specs=[pl.BlockSpec(memory_space=pltpu.HBM)] * 6,
        out_specs=(whole,) * 6,
        scratch_shapes=scratch,
        compiler_params=pltpu.CompilerParams(collective_id=0, has_side_effects=True, vmem_limit_bytes=44 * 2**20),
        name="coupling_step",
    )(*[pltpu.with_memory_space_constraint(v, pltpu.HBM) for v in operands])
    chunk = pl.BlockSpec((8, cy, cz), lambda i: (i, 0, 0))
    return pl.pallas_call(
        finish,
        grid=(cx // 8,),
        out_shape=(out, out),
        in_specs=[whole] * 6,
        out_specs=(chunk, chunk),
        compiler_params=pltpu.CompilerParams(vmem_limit_bytes=16 * 2**20),
        name="finish_step",
    )(*state)


def solution(mesh):
    nx, nz = XCHIPS, mesh.shape["solid"] // CORES
    ny = mesh.shape["fluid"] // nx
    both = ("fluid", "solid")
    block = P("fluid", "solid", None)
    return jax.shard_map(
        functools.partial(per_device, nx, ny, nz),
        mesh=mesh,
        in_specs=(block, block, P(None, both), P(None, both), P(both, None), P(both)),
        out_specs=(block, block),
        check_vma=False,
    )
```

```python
import functools

import jax
import jax.numpy as jnp
from jax import lax
from jax.experimental import pallas as pl
from jax.experimental.pallas import tpu as pltpu
from jax.sharding import PartitionSpec as P

ITERS = 3
XCHIPS = 4
CORES = 2
MESH = pl.DeviceIdType.MESH
F32 = jnp.float32
BF16 = jnp.bfloat16
AROUND = [(a, b) for a in (-1, 0, 1) for b in (-1, 0, 1) if (a, b) != (0, 0)]
LOW = 5
SIDE = 8


def iota(shape, axis):
    return lax.broadcasted_iota(jnp.int32, shape, axis)


def body(
    nx, ny, nz,
    x0_hbm, c_hbm, b_hbm, j_hbm, owner_hbm, slot_hbm,
    field, w0, w1, w2, last, coefs,
    bv, jv, idx, tabs, held, jac, codes, code_own, key, jm, acc,
    part_out, part_in, cross_in, edge, sum_out, sum_plane, sum_line,
    load_sem, bx_send, bx_recv, jx_send, jx_recv, cx_send, cx_recv,
    ring_send, ring_recv, halo_send, halo_recv, row_send, row_recv, cross_send, cross_recv, ar_send, ar_recv, tokens,
):
    xe, de = field.at[0], field.at[1]
    cx, cy, cz = (xe.shape[0] - 10, xe.shape[1] - 16, xe.shape[2])
    quads, faces = bv.shape
    rows = jv.shape[1]
    share = quads // nx
    many = 128 // share
    deep = faces // many
    rowsets = rows // 128
    f, s = lax.axis_index("fluid"), lax.axis_index("solid")
    nf, ns = nx * ny, nz * CORES
    x, y = lax.rem(f, nx), f // nx

    def remote(src, dst, send, recv, at):
        return pltpu.make_async_remote_copy(
            src_ref=src, dst_ref=dst, send_sem=send, recv_sem=recv,
            device_id=at, device_id_type=MESH,
        )

    def beside(a, b):
        return (lax.rem(f + a + nf, nf), lax.rem(s + b + ns, ns))

    def on_x(d):
        return (y * nx + lax.rem(x + d, nx), s)

    def on_y(d):
        return (lax.rem(y + d, ny) * nx + x, s)

    def in_row(a, d, b):
        return (lax.rem(y + a + ny, ny) * nx + lax.rem(x + d, nx), lax.rem(s + b + ns, ns))

    def on_plane(d, e):
        return (lax.rem(y + e, ny) * nx + lax.rem(x + d, nx), s)

    def on_line(n):
        return (f, lax.rem(s + n, ns))

    inner = (pl.ds(LOW, cx), pl.ds(SIDE, cy))
    loads = [
        pltpu.make_async_copy(b_hbm, bv, load_sem.at[0]),
        pltpu.make_async_copy(owner_hbm, idx.at[0], load_sem.at[1]),
        pltpu.make_async_copy(slot_hbm, idx.at[1], load_sem.at[2]),
        pltpu.make_async_copy(j_hbm, jv, load_sem.at[3]),
        pltpu.make_async_copy(x0_hbm, xe.at[inner], load_sem.at[4]),
        pltpu.make_async_copy(c_hbm, de.at[inner], load_sem.at[5]),
    ]
    for load in loads:
        load.start()

    barrier = pltpu.get_barrier_semaphore()
    partners = [on_x(d) for d in range(1, nx)] + [on_y(1), on_y(ny - 1), beside(0, -1), beside(0, 1)]
    for at in partners:
        pl.semaphore_signal(barrier, inc=1, device_id=at, device_id_type=MESH)

    def tell(kind, low, high):
        pl.semaphore_signal(tokens.at[kind, 0], inc=1, device_id=low, device_id_type=MESH)
        pl.semaphore_signal(tokens.at[kind, 1], inc=1, device_id=high, device_id_type=MESH)

    def hear(kind):
        pl.semaphore_wait(tokens.at[kind, 0], 1)
        pl.semaphore_wait(tokens.at[kind, 1], 1)

    guard = jnp.zeros(xe.shape[1:], F32)
    for ref in (xe, w0, w1, w2):
        ref[0] = guard
        ref[cx + 9] = guard

    for end in (0, nx * rowsets + 1):
        part_out[end] = jnp.zeros((1, 128), F32)

    with jax.named_scope("tables"):
        loads[0].wait()
        for a in range(nx):
            mine = bv[a * share : (a + 1) * share, :]
            stack = jnp.concatenate(
                [mine[:, (m * deep // 128) * 128 : (m * deep // 128) * 128 + 128] for m in range(many)], axis=0
            )
            if deep < 128:
                turned = pltpu.roll(stack, 128 - deep, 1)
                odd = (iota(stack.shape, 0) // share) % 2 == 1
                stack = jnp.where(odd, turned, stack)
            tabs[a] = stack.T[:deep]
        loads[1].wait()
        loads[2].wait()
        code_own[...] = idx[0] * faces + idx[1]
        codes[0] = code_own[...]
        held[y, 0] = tabs[x]

    with jax.named_scope("entry"):
        pl.semaphore_wait(barrier, len(partners))
        tell(0, beside(0, -1), beside(0, 1))

    def ring(t, d, way):
        slot = lax.rem(y + ny + (1 - t if way == 0 else t - 1), ny)
        at = on_y(1 if way == 0 else ny - 1)
        block = held.at[slot, d]
        return remote(block, block, ring_send, ring_recv.at[way, t - 1, d], at)

    half = ny // 2

    def goes(t, d, way):
        return t < half or (d < nx // 2) == (way == 0)

    ways = [
        [[ring(t, d, way) if goes(t, d, way) else None for way in range(2)] for d in range(nx)]
        for t in range(1, half + 1)
    ]

    def forward(t, d):
        if t == 1 and d > 0:
            spread[d - 1].wait_recv()
        for way in range(2):
            if t > 1:
                ways[t - 2][d][way].wait_recv()
            if goes(t, d, way):
                ways[t - 1][d][way].start()

    forward(1, 0)
    spread = []
    for d in range(1, nx):
        remote(code_own, codes.at[d], cx_send, cx_recv, on_x(d)).start()
    some = pl.ds(0, nx - 1)
    coded = remote(codes.at[some], codes.at[some], cx_send, cx_recv, on_x(1))
    jacs = remote(jac.at[some], jac.at[some], jx_send, jx_recv, on_x(1))
    spread_all = remote(tabs.at[some], tabs.at[some], bx_send, bx_recv.at[0], on_x(1))
    ring_all = remote(held.at[pl.ds(0, ny - 1)], held.at[pl.ds(0, ny - 1)], ring_send, bx_recv.at[0], on_x(1))
    for d in range(1, nx):
        to = lax.rem(x + d, nx)
        spread.append(remote(tabs.at[to], held.at[y, d], bx_send, bx_recv.at[d - 1], on_x(d)))
        spread[-1].start()

    def prepare_keys(d):
        for i in range(rowsets):
            code = codes[d, i : i + 1, :]
            owner, slot = code // faces, lax.rem(code, faces)
            keys = (owner * deep + lax.rem(slot, deep)).astype(F32)
            key[d * rows + i * 128 : d * rows + (i + 1) * 128, :] = jnp.broadcast_to(keys, (128, 128)).T

    def prepare_jac(d):
        for i in range(rowsets):
            slot = lax.rem(codes[d, i : i + 1, :], faces)
            j = jac[d, :, i * 128 : (i + 1) * 128]
            tiled = jnp.concatenate([j] * many, axis=0)
            wanted = iota((128, 128), 0) // share == jnp.broadcast_to(slot // deep, (128, 128))
            jm[d * rows + i * 128 : d * rows + (i + 1) * 128, :] = jnp.where(wanted, tiled, 0.0).T

    def weight(slot):
        parts = []
        for d in range(nx):
            parts.append(held[slot, d])
        table = jnp.concatenate(parts, axis=0)
        high = table.astype(BF16)
        low = (table - high.astype(F32)).astype(BF16)
        return jnp.concatenate([high, low], axis=1)

    def base_of(slot, d):
        return (slot * nx + lax.rem(x - d + nx, nx)) * deep

    tall = 512

    def pick(d, slots, first=False, finish=None):
        table = jnp.concatenate([weight(slot) for slot in slots], axis=0)
        lanes = iota((1, 128), 1)
        marks = []
        for slot in slots:
            for tile in range(nx * deep // 128):
                mark = jnp.zeros((1, 128), jnp.int32)
                for e in range(128 // deep):
                    p = tile * (128 // deep) + e
                    mark = jnp.where(lanes // deep == e, base_of(slot, p) + lanes - e * deep, mark)
                marks.append(mark.astype(F32))
        for i in range(rows // tall):
            start = d * rows + i * tall
            place = pl.ds(start if isinstance(start, int) else pl.multiple_of(start, tall), tall)
            keys = key[place, :]
            hot = jnp.concatenate([jnp.where(keys == mark, 1.0, 0.0).astype(BF16) for mark in marks], axis=1)
            both = jnp.dot(hot, table, preferred_element_type=F32)
            got = both[:, :128] + both[:, 128:]
            if not first:
                got = got + acc[place, :]
            if finish is None:
                acc[place, :] = got
                continue
            product = got * jm[place, :]
            for k in range(tall // 128):
                line = jnp.sum(product[k * 128 : (k + 1) * 128].T, axis=0, keepdims=True)
                at = i * (tall // 128) + k
                part_out[1 + finish * rowsets + at] = line

    def around_sum(ref, r, n):
        mid = ref[pl.ds(r, n)].reshape(n * xe.shape[1], cz)
        out = ref[pl.ds(r - 1, n)] + ref[pl.ds(r + 1, n)]
        out = out.reshape(n * xe.shape[1], cz)
        out = out + (pltpu.roll(mid, 1, 0) + pltpu.roll(mid, mid.shape[0] - 1, 0))
        lane = iota(mid.shape, 1)
        out = out + jnp.where(lane == 0, 0.0, pltpu.roll(mid, 1, 1))
        out = out + jnp.where(lane == cz - 1, 0.0, pltpu.roll(mid, cz - 1, 1))
        return out.reshape(n, xe.shape[1], cz)

    def start_solid():
        for ref, fill in ((xe, 0.0), (de, 1e30)):
            @pl.when(f == 0)
            def _():
                ref[pl.ds(LOW - 4, 4)] = jnp.full((4,) + xe.shape[1:], fill, F32)

            @pl.when(f == nf - 1)
            def _():
                ref[pl.ds(LOW + cx, 4)] = jnp.full((4,) + xe.shape[1:], fill, F32)

            @pl.when(s == 0)
            def _():
                ref[pl.ds(1, cx + 8), pl.ds(0, 8)] = jnp.full((cx + 8, 8, cz), fill, F32)

            @pl.when(s == ns - 1)
            def _():
                ref[pl.ds(1, cx + 8), pl.ds(SIDE + cy, 8)] = jnp.full((cx + 8, 8, cz), fill, F32)

        def one(i, carry):
            r = 1 + 8 * i
            got = around_sum(xe, r, 8) - 6.0 * xe[pl.ds(r, 8)]
            c = de[pl.ds(r, 8)]
            inverse = jnp.where(c > 1e29, 0.0, 1.0 / (6.0 + c))
            de[pl.ds(r, 8)] = inverse
            w0[pl.ds(r, 8)] = inverse * got
            return carry

        lax.fori_loop(0, (cx + 8) // 8, one, 0)

    order = sorted(range(nx), key=lambda d: (min(d, nx - d), -d))

    def round_of(t):
        others = [(t, d) for d in order if d > 0]
        ahead = [(t + 2, 0)] if t + 2 <= half else []
        return ([(2, 0)] if t == 1 and half > 1 else []) + others + ahead

    prepare_keys(0)
    for n, (t, d) in enumerate(round_of(1)):
        with jax.named_scope(f"forward#t={t}#d={d}"):
            forward(t, d)
        if (t, d) == (1, order[1]):
            coded.wait_recv()
        if t == 1:
            prepare_keys(d)
    with jax.named_scope("hear#k=0"):
        hear(0)
        for load in loads[3:]:
            load.wait()
        jac[0] = jv[pl.ds(pl.multiple_of(x * share, share), share), :]
    tell(1, on_y(ny - 1), on_y(1))
    if ns > 4:
        tell(2, beside(0, -2), beside(0, 2))
    for d in range(1, nx):
        to = lax.rem(x + d, nx)
        remote(
            jv.at[pl.ds(pl.multiple_of(to * share, share), share)], jac.at[d], jx_send, jx_recv, on_x(d)
        ).start()
    to_y = {-1: (pl.ds(SIDE, 8), pl.ds(SIDE + cy, 8)), 0: (pl.ds(SIDE, cy),) * 2, 1: (pl.ds(SIDE + cy - 8, 8), pl.ds(SIDE - 8, 8))}

    def send_side(a):
        def rows_of(count):
            if a == 1:
                return pl.ds(LOW + cx - count, count), pl.ds(LOW - count, count)
            return pl.ds(LOW, count), pl.ds(LOW + cx, count)

        near, near_to = rows_of(3)
        four, four_to = rows_of(4)
        fourth = pl.ds(LOW + cx - 4 if a == 1 else LOW + 3, 1)
        fourth_to = pl.ds(LOW - 4 if a == 1 else LOW + cx + 3, 1)
        sides = pl.ds(SIDE, cy)
        cuts = [
            (field.at[:, near, sides], field.at[:, near_to, sides], 1, 0),
            (field.at[0, fourth, sides], field.at[0, fourth_to, sides], 2, 0),
            (field.at[:, near, pl.ds(SIDE + cy - 4, 4)], field.at[:, near_to, pl.ds(SIDE - 4, 4)], 3, 1),
            (field.at[:, near, pl.ds(SIDE, 4)], field.at[:, near_to, pl.ds(SIDE + cy, 4)], 3, -1),
        ]
        for src, dst, k, b in cuts:
            remote(src, dst, halo_send.at[k], halo_recv.at[k], beside(a, b)).start()

    ends = ((1, nx - 1), (-1, 0))

    def send_sides(inside):
        for a, end in ends:
            @pl.when((x != end) if inside else (x == end))
            def _():
                send_side(a)

    for b in (-1, 1):
        remote(
            field.at[:, pl.ds(LOW, cx), to_y[b][0]], field.at[:, pl.ds(LOW, cx), to_y[b][1]],
            halo_send.at[0], halo_recv.at[0], beside(0, b),
        ).start()
    send_sides(True)
    rims = [
        field.at[:, pl.ds(LOW, cx), pl.ds(0, 16)],
        field.at[:, pl.ds(LOW - 3, 6), pl.ds(SIDE, cy)],
        field.at[0, pl.ds(LOW - 4, 2), pl.ds(SIDE, cy)],
        field.at[:, pl.ds(LOW - 3, 6), pl.ds(0, 8)],
    ]
    halos = [remote(rim, rim, halo_send.at[k], halo_recv.at[k], on_x(1)) for k, rim in enumerate(rims)]

    def near(far):
        if far == 0:
            return [y]
        return [lax.rem(y + ny - far, ny), lax.rem(y + far, ny)]

    unprepared = list(order)

    def next_jac():
        with jax.named_scope(f"prepare_jac#n={len(unprepared)}"):
            if len(unprepared) == nx:
                jacs.wait_recv()
            prepare_jac(unprepared.pop(0))

    def hear_more():
        hear(1)
        if ns > 4:
            hear(2)
        if ns > 8:
            tell(3, beside(0, -4), beside(0, 4))

    for t in range(2, half + 1):
        todo = round_of(t)
        for n, d in enumerate(order):
            if n < len(todo):
                with jax.named_scope(f"forward#t={t}#n={n}"):
                    forward(*todo[n])
            with jax.named_scope(f"pick#t={t}#d={d}"):
                pick(d, near(t - 2), first=t == 2)
            if t == max(2, half - 1) and n == 0:
                hear_more()
            if (t == half - 1 and n % 2 == 1) or (t == half and n < 2):
                next_jac()
    send_sides(False)
    if half == 1:
        hear_more()
    while unprepared:
        next_jac()
    for d in range(nx):
        with jax.named_scope(f"pick_near#d={d}"):
            pick(d, near(half - 1), first=half == 1)
    if ns > 8:
        with jax.named_scope("hear#k=3"):
            hear(3)
    with jax.named_scope("far_wait"):
        for d in range(nx):
            for way in range(2):
                if goes(half, d, way):
                    ways[half - 1][d][way].wait_recv()
    def share_ends(b):
        slot = (1 - b) * nx + x
        line = part_out.at[nx * rowsets]
        remote(line, cross_in.at[0, slot], cross_send, cross_recv.at[0], in_row(1, nx - x, b)).start()
        line = part_out.at[1]
        remote(line, cross_in.at[1, slot], cross_send, cross_recv.at[1], in_row(-1, 2 * nx - 1 - x, b)).start()

    def share_rows(b):
        slot = (1 - b) * nx + x
        for d in order[::-1]:
            if (d, b) != (0, 0):
                lines = part_out.at[pl.ds(lax.rem(x + d, nx) * rowsets, rowsets + 2)]
                remote(lines, part_in.at[slot], row_send, row_recv, in_row(0, d, b)).start()

    readers = [0, nx - 1] + list(range(1, nx - 1))
    for n, reader in enumerate(readers):
        with jax.named_scope(f"pick_far#d={reader}"):
            pick(lax.rem(x - reader + nx, nx), [lax.rem(y + half, ny)], finish=reader)
        if n == 2:
            for b in (1, -1, 0):
                share_ends(b)
    for b in (1, -1, 0):
        share_rows(b)
    part_in[nx + x] = part_out[pl.ds(x * rowsets, rowsets + 2)]
    most = part_in.at[pl.ds(0, 3 * nx - 1)]
    rows_all = remote(most, most, row_send, row_recv, on_x(1))
    six = cross_in.at[0, pl.ds(0, 6)]
    cross_all = remote(six, six, cross_send, cross_recv.at[0], on_x(1))
    with jax.named_scope("solid_wait"):
        for halo in halos:
            halo.wait_send()
        for halo in halos:
            halo.wait_recv()
    with jax.named_scope("solid_start"):
        start_solid()
    with jax.named_scope("part_wait"):
        rows_all.wait_recv()
        for side, end in ((0, 0), (1, nx - 1)):
            @pl.when(x == end)
            def _():
                whole = cross_in.at[side]
                remote(whole, whole, cross_send, cross_recv.at[side], on_x(1)).wait_recv()

    per = 128 // cy

    def heat(r, first, count, line, offset):
        shape = (per, count, 128)
        spot = iota(shape, 2)
        picked = jnp.where(spot == iota(shape, 0) * cy + iota(shape, 1) + offset, line.reshape(1, 1, 128), 0.0)
        column = jnp.sum(picked, axis=2, keepdims=True)
        here = (pl.ds(r, per), pl.ds(first, count))
        w0[here] = w0[here] + jnp.where(spot == cz - 1, column * de[here], 0.0)

    def gathered(b, spot):
        return sum(part_in[(b + 1) * nx + h, spot] for h in range(nx))

    with jax.named_scope("heat"):
        for a, end, side, spot in ((1, nx - 1, 1, rowsets + 1), (-1, 0, 0, 0)):
            for b in (-1, 0, 1):
                here = pl.ds(3 * side + b + 1, 1)

                @pl.when(x == end)
                def _():
                    edge[here, :] = sum(cross_in[side, (b + 1) * nx + h] for h in range(nx))

                @pl.when(x != end)
                def _():
                    edge[here, :] = gathered(b, spot)

        for a in (-1, 0, 1):
            for b in (-1, 0, 1):
                first = {0: SIDE, -1: 0, 1: SIDE + cy}[b]
                count = {0: cy, -1: 8, 1: 8}[b]
                offset = {0: 0, -1: cy - 8, 1: 0}[b]
                if a == 0:
                    for i in range(cx // per):
                        heat(LOW + i * per, first, count, gathered(b, 1 + i), offset)
                else:
                    at = 3 * (1 if a == 1 else 0) + b + 1
                    heat(LOW + cx if a == 1 else LOW - 4, first, count, edge[at : at + 1, :], offset)

    def fold(v):
        return jnp.sum(v.reshape(-1, 8, cz), axis=0)

    def inside(v):
        return v[:, SIDE : SIDE + cy]

    def step(ref, new, first):
        def one(i, carry):
            r = LOW + 8 * i
            near = around_sum(ref, r, 8)
            inverse = de[pl.ds(r, 8)]
            new_w = inverse * near
            new[pl.ds(r, 8)] = new_w
            now = inside(ref[pl.ds(r, 8)])
            near = inside(near)
            odd = carry[0] + fold(now * near)
            even = carry[1] + fold(inside(new_w) * near)
            if first:
                return (odd, even, carry[2] + fold(now * now / inside(inverse)))
            return (odd, even)

        zero = jnp.zeros((8, cz), F32)
        sums = lax.fori_loop(0, cx // 8, one, (zero,) * (3 if first else 2), unroll=True)
        for r in (LOW - 4, LOW + cx):
            new[pl.ds(r, 4)] = de[pl.ds(r, 4)] * around_sum(ref, r, 4)
        return sums

    with jax.named_scope("step#k=0"):
        mu1, mu2, mu0 = step(w0, w1, True)
    with jax.named_scope("step#k=1"):
        mu3, mu4 = step(w1, w2, False)

    def final(i, carry):
        near = inside(around_sum(w2, LOW + 8 * i, 8))
        last[pl.ds(8 * i, 8)] = near
        return carry + fold(inside(w2[pl.ds(LOW + 8 * i, 8)]) * near)

    with jax.named_scope("step#k=2"):
        mu5 = lax.fori_loop(0, cx // 8, final, jnp.zeros((8, cz), F32), unroll=True)
    lines = [jnp.sum(v, axis=0, keepdims=True) for v in (mu0, mu1, mu2, mu3, mu4, mu5)]
    lines.append(jnp.zeros((2, cz), F32))
    sums = jnp.sum(jnp.concatenate(lines, axis=0), axis=1, keepdims=True)
    local = jnp.sum(jnp.where(iota((8, 128), 0) == iota((8, 128), 1), sums, 0.0), axis=0, keepdims=True)
    sends = []

    def reduce(stage, value, slots, me, peers):
        sum_out[stage] = value
        slots[me] = value
        for at in peers:
            remote(sum_out.at[stage], slots.at[me], ar_send.at[stage], ar_recv.at[stage], at).start()
        every = slots.at[pl.ds(0, len(peers))]
        everyone = remote(every, every, ar_send.at[stage], ar_recv.at[stage], peers[0])
        everyone.wait_recv()
        sends.append(everyone)
        return jnp.sum(slots[...], axis=0)

    others = [(d, e) for d in range(nx) for e in range(ny) if (d, e) != (0, 0)]
    others.sort(key=lambda o: -min(o[0], nx - o[0]) - min(o[1], ny - o[1]))
    far_first = sorted(range(1, ns), key=lambda n: -min(n, ns - n))
    with jax.named_scope("reduce#k=0"):
        local = reduce(0, local, sum_plane, f, [on_plane(d, e) for d, e in others])
    with jax.named_scope("reduce#k=1"):
        local = reduce(1, local, sum_line, s, [on_line(n) for n in far_first])
    lane = iota((1, 128), 1)
    mu = [jnp.sum(jnp.where(lane == k, local, 0.0), axis=1, keepdims=True) for k in range(6)]
    mu = [jnp.broadcast_to(m, (1, 128)) for m in mu]

    def product(u, v):
        out = 0.0
        for a, left in enumerate(u):
            for b, right in enumerate(v):
                out = out + left * right * mu[a + b]
        return out

    one_line = jnp.ones((1, cz), F32)
    course, misfit, guess = [one_line], [one_line], []
    rz = mu[0]
    for it in range(ITERS):
        image = [
            (course[k] if k < len(course) else 0.0) - (course[k - 1] if k > 0 else 0.0)
            for k in range(len(course) + 1)
        ]
        alpha = rz / product(course, image)
        guess = [(guess[k] if k < len(guess) else 0.0) + alpha * course[k] for k in range(len(course))]
        misfit = [(misfit[k] if k < len(misfit) else 0.0) - alpha * image[k] for k in range(len(image))]
        if it + 1 < ITERS:
            new = product(misfit, misfit)
            ratio = new / rz
            course = [misfit[k] + (ratio * course[k] if k < len(course) else 0.0) for k in range(len(misfit))]
            rz = new

    coefs[...] = jnp.concatenate(guess + misfit + [one_line], axis=0)
    with jax.named_scope("sent"):
        for copy in [spread_all, coded, jacs, ring_all, rows_all, cross_all] + sends:
            copy.wait_send()


def finish(field, w0, w1, w2, last, coefs, guess, misfit):
    xe, de = field.at[0], field.at[1]
    n, cy, _ = guess.shape
    first = pl.program_id(0) * n
    here = (pl.ds(LOW + first, n), pl.ds(SIDE, cy))
    line = [coefs[k : k + 1, :] for k in range(7)]
    basis = [w0[here], w1[here], w2[here]]
    guess[...] = xe[here] + (line[0] * basis[0] + (line[1] * basis[1] + line[2] * basis[2]))
    rest = line[3] * basis[0] + (line[4] * basis[1] + line[5] * basis[2])
    misfit[...] = rest / de[here] + line[6] * last[pl.ds(first, n)]


def per_device(nx, ny, nz, x0, c, b, j, owner, slot):
    quads, faces = b.shape
    rows = slot.shape[0]
    cx, cy, cz = x0.shape
    share = quads // nx
    deep = faces * share // 128
    half = ny // 2
    wide = (cx + 10, cy + 16, cz)
    lines = rows // 128
    nf, ns = nx * ny, nz * CORES
    dma = pltpu.SemaphoreType.DMA
    vmem = pltpu.VMEM
    scratch = [
        vmem((quads, faces), F32), vmem((quads, rows), F32), vmem((2, lines, 128), jnp.int32),
        vmem((nx, deep, 128), F32), vmem((ny, nx, deep, 128), F32), vmem((nx, share, rows), F32),
        vmem((nx, lines, 128), jnp.int32), vmem((lines, 128), jnp.int32),
        vmem((nx * rows, 128), F32), vmem((nx * rows, 128), F32), vmem((nx * rows, 128), F32),
        vmem((nx * lines + 2, 1, 128), F32), vmem((3 * nx, lines + 2, 1, 128), F32), vmem((2, 3 * nx, 1, 128), F32), vmem((8, 128), F32),
        vmem((2, 1, 128), F32), vmem((nf, 1, 128), F32), vmem((ns, 1, 128), F32),
        dma((6,)), dma, dma((nx - 1,)), dma, dma, dma, dma,
        dma, dma((2, half, nx)), dma((4,)), dma((4,)), dma, dma, dma, dma((2,)), dma((2,)), dma((2,)),
        pltpu.SemaphoreType.REGULAR((4, 2)),
    ]
    wide_out = jax.ShapeDtypeStruct(wide, F32)
    out = jax.ShapeDtypeStruct((cx, cy, cz), F32)
    whole = pl.BlockSpec(memory_space=vmem)
    operands = (x0, c, b, j, owner.reshape(lines, 128), slot.reshape(lines, 128))
    state = pl.pallas_call(
        functools.partial(body, nx, ny, nz),
        out_shape=(jax.ShapeDtypeStruct((2,) + wide, F32),) + (wide_out,) * 3 + (out, jax.ShapeDtypeStruct((8, 128), F32)),
        in_specs=[pl.BlockSpec(memory_space=pltpu.HBM)] * 6,
        out_specs=(whole,) * 6,
        scratch_shapes=scratch,
        compiler_params=pltpu.CompilerParams(collective_id=0, has_side_effects=True, vmem_limit_bytes=44 * 2**20),
        name="coupling_step",
    )(*[pltpu.with_memory_space_constraint(v, pltpu.HBM) for v in operands])
    chunk = pl.BlockSpec((8, cy, cz), lambda i: (i, 0, 0))
    return pl.pallas_call(
        finish,
        grid=(cx // 8,),
        out_shape=(out, out),
        in_specs=[whole] * 6,
        out_specs=(chunk, chunk),
        compiler_params=pltpu.CompilerParams(vmem_limit_bytes=16 * 2**20),
        name="finish_step",
    )(*state)


def solution(mesh):
    nx, nz = XCHIPS, mesh.shape["solid"] // CORES
    ny = mesh.shape["fluid"] // nx
    both = ("fluid", "solid")
    block = P("fluid", "solid", None)
    return jax.shard_map(
        functools.partial(per_device, nx, ny, nz),
        mesh=mesh,
        in_specs=(block, block, P(None, both), P(None, both), P(both, None), P(both)),
        out_specs=(block, block),
        check_vma=False,
    )
```

```python
import functools

import jax
import jax.numpy as jnp
from jax import lax
from jax.experimental import pallas as pl
from jax.experimental.pallas import tpu as pltpu
from jax.sharding import PartitionSpec as P

ITERS = 3
XCHIPS = 4
CORES = 2
MESH = pl.DeviceIdType.MESH
F32 = jnp.float32
BF16 = jnp.bfloat16
AROUND = [(a, b) for a in (-1, 0, 1) for b in (-1, 0, 1) if (a, b) != (0, 0)]
LOW = 5
SIDE = 8


def iota(shape, axis):
    return lax.broadcasted_iota(jnp.int32, shape, axis)


def body(
    nx, ny, nz,
    x0_hbm, c_hbm, b_hbm, j_hbm, owner_hbm, slot_hbm,
    field, w0, w1, w2, last, coefs,
    bv, jv, idx, tabs, held, jac, codes, code_own, key, jm, acc,
    part_out, part_in, cross_in, edge, sum_out, sum_plane, sum_line,
    load_sem, bx_send, bx_recv, jx_send, jx_recv, cx_send, cx_recv,
    ring_send, ring_recv, halo_send, halo_recv, row_send, row_recv, cross_send, cross_recv, ar_send, ar_recv, tokens, tables,
):
    xe, de = field.at[0], field.at[1]
    cx, cy, cz = (xe.shape[0] - 10, xe.shape[1] - 16, xe.shape[2])
    quads, faces = bv.shape
    rows = jv.shape[1]
    share = quads // nx
    many = 128 // share
    deep = faces // many
    rowsets = rows // 128
    f, s = lax.axis_index("fluid"), lax.axis_index("solid")
    nf, ns = nx * ny, nz * CORES
    x, y = lax.rem(f, nx), f // nx

    def remote(src, dst, send, recv, at):
        return pltpu.make_async_remote_copy(
            src_ref=src, dst_ref=dst, send_sem=send, recv_sem=recv,
            device_id=at, device_id_type=MESH,
        )

    def beside(a, b):
        return (lax.rem(f + a + nf, nf), lax.rem(s + b + ns, ns))

    def on_x(d):
        return (y * nx + lax.rem(x + d, nx), s)

    def on_y(d):
        return (lax.rem(y + d, ny) * nx + x, s)

    def in_row(a, d, b):
        return (lax.rem(y + a + ny, ny) * nx + lax.rem(x + d, nx), lax.rem(s + b + ns, ns))

    def on_plane(d, e):
        return (lax.rem(y + e, ny) * nx + lax.rem(x + d, nx), s)

    def on_line(n):
        return (f, lax.rem(s + n, ns))

    inner = (pl.ds(LOW, cx), pl.ds(SIDE, cy))
    loads = [
        pltpu.make_async_copy(b_hbm, bv, load_sem.at[0]),
        pltpu.make_async_copy(owner_hbm, idx.at[0], load_sem.at[1]),
        pltpu.make_async_copy(slot_hbm, idx.at[1], load_sem.at[2]),
        pltpu.make_async_copy(j_hbm, jv, load_sem.at[3]),
        pltpu.make_async_copy(x0_hbm, xe.at[inner], load_sem.at[4]),
        pltpu.make_async_copy(c_hbm, de.at[inner], load_sem.at[5]),
    ]
    for load in loads:
        load.start()

    barrier = pltpu.get_barrier_semaphore()
    partners = [on_x(d) for d in range(1, nx)] + [on_y(1), on_y(ny - 1), beside(0, -1), beside(0, 1)]
    for at in partners:
        pl.semaphore_signal(barrier, inc=1, device_id=at, device_id_type=MESH)

    def tell(kind, low, high):
        pl.semaphore_signal(tokens.at[kind, 0], inc=1, device_id=low, device_id_type=MESH)
        pl.semaphore_signal(tokens.at[kind, 1], inc=1, device_id=high, device_id_type=MESH)

    def hear(kind):
        pl.semaphore_wait(tokens.at[kind, 0], 1)
        pl.semaphore_wait(tokens.at[kind, 1], 1)

    guard = jnp.zeros(xe.shape[1:], F32)
    for ref in (xe, w0, w1, w2):
        ref[0] = guard
        ref[cx + 9] = guard

    for end in (0, nx * rowsets + 1):
        part_out[end] = jnp.zeros((1, 128), F32)

    with jax.named_scope("tables"):
        loads[0].wait()
        for a in range(nx):
            mine = bv[a * share : (a + 1) * share, :]
            stack = jnp.concatenate(
                [mine[:, (m * deep // 128) * 128 : (m * deep // 128) * 128 + 128] for m in range(many)], axis=0
            )
            if deep < 128:
                turned = pltpu.roll(stack, 128 - deep, 1)
                odd = (iota(stack.shape, 0) // share) % 2 == 1
                stack = jnp.where(odd, turned, stack)
            tabs[a] = stack.T[:deep]
        loads[1].wait()
        loads[2].wait()
        code_own[...] = idx[0] * faces + idx[1]
        codes[0] = code_own[...]
        held[y, 0] = tabs[x]

    with jax.named_scope("entry"):
        pl.semaphore_wait(barrier, len(partners))
        tell(0, beside(0, -1), beside(0, 1))

    def ring(t, d, way):
        slot = lax.rem(y + ny + (1 - t if way == 0 else t - 1), ny)
        at = on_y(1 if way == 0 else ny - 1)
        block = held.at[slot, d]
        return remote(block, block, ring_send, ring_recv.at[way, t - 1, d], at)

    half = ny // 2

    def goes(t, d, way):
        return t < half or (d < nx // 2) == (way == 0)

    ways = [
        [[ring(t, d, way) if goes(t, d, way) else None for way in range(2)] for d in range(nx)]
        for t in range(1, half + 1)
    ]

    def forward(t, d):
        if t == 1 and d > 0:
            spread[d - 1].wait_recv()
        for way in range(2):
            if t > 1:
                ways[t - 2][d][way].wait_recv()
            if goes(t, d, way):
                ways[t - 1][d][way].start()

    forward(1, 0)
    spread = []
    for d in range(1, nx):
        remote(code_own, codes.at[d], cx_send, cx_recv, on_x(d)).start()
    some = pl.ds(0, nx - 1)
    coded = remote(codes.at[some], codes.at[some], cx_send, cx_recv, on_x(1))
    jacs = remote(jac.at[some], jac.at[some], jx_send, jx_recv, on_x(1))
    spread_all = remote(tabs.at[some], tabs.at[some], bx_send, bx_recv.at[0], on_x(1))
    ring_all = remote(held.at[pl.ds(0, ny - 1)], held.at[pl.ds(0, ny - 1)], ring_send, bx_recv.at[0], on_x(1))
    for d in range(1, nx):
        to = lax.rem(x + d, nx)
        spread.append(remote(tabs.at[to], held.at[y, d], bx_send, bx_recv.at[d - 1], on_x(d)))
        spread[-1].start()

    def prepare_keys(d):
        for i in range(rowsets):
            code = codes[d, i : i + 1, :]
            owner, slot = code // faces, lax.rem(code, faces)
            keys = (owner * deep + lax.rem(slot, deep)).astype(F32)
            key[d * rows + i * 128 : d * rows + (i + 1) * 128, :] = jnp.broadcast_to(keys, (128, 128)).T

    def prepare_jac(d):
        for i in range(rowsets):
            slot = lax.rem(codes[d, i : i + 1, :], faces)
            j = jac[d, :, i * 128 : (i + 1) * 128]
            tiled = jnp.concatenate([j] * many, axis=0)
            wanted = iota((128, 128), 0) // share == jnp.broadcast_to(slot // deep, (128, 128))
            jm[d * rows + i * 128 : d * rows + (i + 1) * 128, :] = jnp.where(wanted, tiled, 0.0).T

    def weight(slot):
        parts = []
        for d in range(nx):
            parts.append(held[slot, d])
        table = jnp.concatenate(parts, axis=0)
        high = table.astype(BF16)
        low = (table - high.astype(F32)).astype(BF16)
        return jnp.concatenate([high, low], axis=1)

    def base_of(slot, d):
        return (slot * nx + lax.rem(x - d + nx, nx)) * deep

    tall = 512

    def pick(d, slots, fresh, first=False, finish=None):
        if fresh:
            for n, slot in enumerate(slots):
                tables[n * nx * deep : (n + 1) * nx * deep, :] = weight(slot)
        table = tables[: len(slots) * nx * deep, :]
        lanes = iota((1, 128), 1)
        marks = []
        for slot in slots:
            for tile in range(nx * deep // 128):
                mark = jnp.zeros((1, 128), jnp.int32)
                for e in range(128 // deep):
                    p = tile * (128 // deep) + e
                    mark = jnp.where(lanes // deep == e, base_of(slot, p) + lanes - e * deep, mark)
                marks.append(mark.astype(F32))
        for i in range(rows // tall):
            start = d * rows + i * tall
            place = pl.ds(start if isinstance(start, int) else pl.multiple_of(start, tall), tall)
            keys = key[place, :]
            hot = jnp.concatenate([jnp.where(keys == mark, 1.0, 0.0).astype(BF16) for mark in marks], axis=1)
            both = jnp.dot(hot, table, preferred_element_type=F32)
            got = both[:, :128] + both[:, 128:]
            if not first:
                got = got + acc[place, :]
            if finish is None:
                acc[place, :] = got
                continue
            product = got * jm[place, :]
            for k in range(tall // 128):
                line = jnp.sum(product[k * 128 : (k + 1) * 128].T, axis=0, keepdims=True)
                at = i * (tall // 128) + k
                part_out[1 + finish * rowsets + at] = line

    def around_sum(ref, r, n):
        mid = ref[pl.ds(r, n)].reshape(n * xe.shape[1], cz)
        out = ref[pl.ds(r - 1, n)] + ref[pl.ds(r + 1, n)]
        out = out.reshape(n * xe.shape[1], cz)
        out = out + (pltpu.roll(mid, 1, 0) + pltpu.roll(mid, mid.shape[0] - 1, 0))
        lane = iota(mid.shape, 1)
        out = out + jnp.where(lane == 0, 0.0, pltpu.roll(mid, 1, 1))
        out = out + jnp.where(lane == cz - 1, 0.0, pltpu.roll(mid, cz - 1, 1))
        return out.reshape(n, xe.shape[1], cz)

    def start_solid():
        for ref, fill in ((xe, 0.0), (de, 1e30)):
            @pl.when(f == 0)
            def _():
                ref[pl.ds(LOW - 4, 4)] = jnp.full((4,) + xe.shape[1:], fill, F32)

            @pl.when(f == nf - 1)
            def _():
                ref[pl.ds(LOW + cx, 4)] = jnp.full((4,) + xe.shape[1:], fill, F32)

            @pl.when(s == 0)
            def _():
                ref[pl.ds(1, cx + 8), pl.ds(0, 8)] = jnp.full((cx + 8, 8, cz), fill, F32)

            @pl.when(s == ns - 1)
            def _():
                ref[pl.ds(1, cx + 8), pl.ds(SIDE + cy, 8)] = jnp.full((cx + 8, 8, cz), fill, F32)

        def one(i, carry):
            r = 1 + 8 * i
            got = around_sum(xe, r, 8) - 6.0 * xe[pl.ds(r, 8)]
            c = de[pl.ds(r, 8)]
            inverse = jnp.where(c > 1e29, 0.0, 1.0 / (6.0 + c))
            de[pl.ds(r, 8)] = inverse
            w0[pl.ds(r, 8)] = inverse * got
            return carry

        lax.fori_loop(0, (cx + 8) // 8, one, 0)

    order = sorted(range(nx), key=lambda d: (min(d, nx - d), -d))

    def round_of(t):
        others = [(t, d) for d in order if d > 0]
        ahead = [(t + 2, 0)] if t + 2 <= half else []
        return ([(2, 0)] if t == 1 and half > 1 else []) + others + ahead

    prepare_keys(0)
    for n, (t, d) in enumerate(round_of(1)):
        with jax.named_scope(f"forward#t={t}#d={d}"):
            forward(t, d)
        if (t, d) == (1, order[1]):
            coded.wait_recv()
        if t == 1:
            prepare_keys(d)
    with jax.named_scope("hear#k=0"):
        hear(0)
        for load in loads[3:]:
            load.wait()
        jac[0] = jv[pl.ds(pl.multiple_of(x * share, share), share), :]
    tell(1, on_y(ny - 1), on_y(1))
    if ns > 4:
        tell(2, beside(0, -2), beside(0, 2))
    for d in range(1, nx):
        to = lax.rem(x + d, nx)
        remote(
            jv.at[pl.ds(pl.multiple_of(to * share, share), share)], jac.at[d], jx_send, jx_recv, on_x(d)
        ).start()
    to_y = {-1: (pl.ds(SIDE, 8), pl.ds(SIDE + cy, 8)), 0: (pl.ds(SIDE, cy),) * 2, 1: (pl.ds(SIDE + cy - 8, 8), pl.ds(SIDE - 8, 8))}

    def send_side(a):
        def rows_of(count):
            if a == 1:
                return pl.ds(LOW + cx - count, count), pl.ds(LOW - count, count)
            return pl.ds(LOW, count), pl.ds(LOW + cx, count)

        near, near_to = rows_of(3)
        four, four_to = rows_of(4)
        fourth = pl.ds(LOW + cx - 4 if a == 1 else LOW + 3, 1)
        fourth_to = pl.ds(LOW - 4 if a == 1 else LOW + cx + 3, 1)
        sides = pl.ds(SIDE, cy)
        cuts = [
            (field.at[:, near, sides], field.at[:, near_to, sides], 1, 0),
            (field.at[0, fourth, sides], field.at[0, fourth_to, sides], 2, 0),
            (field.at[:, near, pl.ds(SIDE + cy - 4, 4)], field.at[:, near_to, pl.ds(SIDE - 4, 4)], 3, 1),
            (field.at[:, near, pl.ds(SIDE, 4)], field.at[:, near_to, pl.ds(SIDE + cy, 4)], 3, -1),
        ]
        for src, dst, k, b in cuts:
            remote(src, dst, halo_send.at[k], halo_recv.at[k], beside(a, b)).start()

    ends = ((1, nx - 1), (-1, 0))

    def send_sides(inside):
        for a, end in ends:
            @pl.when((x != end) if inside else (x == end))
            def _():
                send_side(a)

    for b in (-1, 1):
        remote(
            field.at[:, pl.ds(LOW, cx), to_y[b][0]], field.at[:, pl.ds(LOW, cx), to_y[b][1]],
            halo_send.at[0], halo_recv.at[0], beside(0, b),
        ).start()
    send_sides(True)
    rims = [
        field.at[:, pl.ds(LOW, cx), pl.ds(0, 16)],
        field.at[:, pl.ds(LOW - 3, 6), pl.ds(SIDE, cy)],
        field.at[0, pl.ds(LOW - 4, 2), pl.ds(SIDE, cy)],
        field.at[:, pl.ds(LOW - 3, 6), pl.ds(0, 8)],
    ]
    halos = [remote(rim, rim, halo_send.at[k], halo_recv.at[k], on_x(1)) for k, rim in enumerate(rims)]

    def near(far):
        if far == 0:
            return [y]
        return [lax.rem(y + ny - far, ny), lax.rem(y + far, ny)]

    unprepared = list(order)

    def next_jac():
        with jax.named_scope(f"prepare_jac#n={len(unprepared)}"):
            if len(unprepared) == nx:
                jacs.wait_recv()
            prepare_jac(unprepared.pop(0))

    def hear_more():
        hear(1)
        if ns > 4:
            hear(2)
        if ns > 8:
            tell(3, beside(0, -4), beside(0, 4))

    for t in range(2, half + 1):
        todo = round_of(t)
        for n, d in enumerate(order):
            if n < len(todo):
                with jax.named_scope(f"forward#t={t}#n={n}"):
                    forward(*todo[n])
            with jax.named_scope(f"pick#t={t}#d={d}"):
                pick(d, near(t - 2), n == 0, first=t == 2)
            if t == max(2, half - 1) and n == 0:
                hear_more()
            if (t == half - 1 and n % 2 == 1) or (t == half and n < 2):
                next_jac()
    send_sides(False)
    if half == 1:
        hear_more()
    while unprepared:
        next_jac()
    for d in range(nx):
        with jax.named_scope(f"pick_near#d={d}"):
            pick(d, near(half - 1), d == 0, first=half == 1)
    if ns > 8:
        with jax.named_scope("hear#k=3"):
            hear(3)
    with jax.named_scope("far_wait"):
        for d in range(nx):
            for way in range(2):
                if goes(half, d, way):
                    ways[half - 1][d][way].wait_recv()
    def share_ends(b):
        slot = (1 - b) * nx + x
        line = part_out.at[nx * rowsets]
        remote(line, cross_in.at[0, slot], cross_send, cross_recv.at[0], in_row(1, nx - x, b)).start()
        line = part_out.at[1]
        remote(line, cross_in.at[1, slot], cross_send, cross_recv.at[1], in_row(-1, 2 * nx - 1 - x, b)).start()

    def share_rows(b):
        slot = (1 - b) * nx + x
        for d in order[::-1]:
            if (d, b) != (0, 0):
                lines = part_out.at[pl.ds(lax.rem(x + d, nx) * rowsets, rowsets + 2)]
                remote(lines, part_in.at[slot], row_send, row_recv, in_row(0, d, b)).start()

    readers = [0, nx - 1] + list(range(1, nx - 1))
    for n, reader in enumerate(readers):
        with jax.named_scope(f"pick_far#d={reader}"):
            pick(lax.rem(x - reader + nx, nx), [lax.rem(y + half, ny)], n == 0, finish=reader)
        if n == 2:
            for b in (1, -1, 0):
                share_ends(b)
    for b in (1, -1, 0):
        share_rows(b)
    part_in[nx + x] = part_out[pl.ds(x * rowsets, rowsets + 2)]
    most = part_in.at[pl.ds(0, 3 * nx - 1)]
    rows_all = remote(most, most, row_send, row_recv, on_x(1))
    six = cross_in.at[0, pl.ds(0, 6)]
    cross_all = remote(six, six, cross_send, cross_recv.at[0], on_x(1))
    with jax.named_scope("solid_wait"):
        for halo in halos:
            halo.wait_send()
        for halo in halos:
            halo.wait_recv()
    with jax.named_scope("solid_start"):
        start_solid()
    with jax.named_scope("part_wait"):
        rows_all.wait_recv()
        for side, end in ((0, 0), (1, nx - 1)):
            @pl.when(x == end)
            def _():
                whole = cross_in.at[side]
                remote(whole, whole, cross_send, cross_recv.at[side], on_x(1)).wait_recv()

    per = 128 // cy

    def heat(r, first, count, line, offset):
        shape = (per, count, 128)
        spot = iota(shape, 2)
        picked = jnp.where(spot == iota(shape, 0) * cy + iota(shape, 1) + offset, line.reshape(1, 1, 128), 0.0)
        column = jnp.sum(picked, axis=2, keepdims=True)
        here = (pl.ds(r, per), pl.ds(first, count))
        w0[here] = w0[here] + jnp.where(spot == cz - 1, column * de[here], 0.0)

    def gathered(b, spot):
        return sum(part_in[(b + 1) * nx + h, spot] for h in range(nx))

    with jax.named_scope("heat"):
        for a, end, side, spot in ((1, nx - 1, 1, rowsets + 1), (-1, 0, 0, 0)):
            for b in (-1, 0, 1):
                here = pl.ds(3 * side + b + 1, 1)

                @pl.when(x == end)
                def _():
                    edge[here, :] = sum(cross_in[side, (b + 1) * nx + h] for h in range(nx))

                @pl.when(x != end)
                def _():
                    edge[here, :] = gathered(b, spot)

        for a in (-1, 0, 1):
            for b in (-1, 0, 1):
                first = {0: SIDE, -1: 0, 1: SIDE + cy}[b]
                count = {0: cy, -1: 8, 1: 8}[b]
                offset = {0: 0, -1: cy - 8, 1: 0}[b]
                if a == 0:
                    for i in range(cx // per):
                        heat(LOW + i * per, first, count, gathered(b, 1 + i), offset)
                else:
                    at = 3 * (1 if a == 1 else 0) + b + 1
                    heat(LOW + cx if a == 1 else LOW - 4, first, count, edge[at : at + 1, :], offset)

    def fold(v):
        return jnp.sum(v.reshape(-1, 8, cz), axis=0)

    def inside(v):
        return v[:, SIDE : SIDE + cy]

    def step(ref, new, first):
        def one(i, carry):
            r = LOW + 8 * i
            near = around_sum(ref, r, 8)
            inverse = de[pl.ds(r, 8)]
            new_w = inverse * near
            new[pl.ds(r, 8)] = new_w
            now = inside(ref[pl.ds(r, 8)])
            near = inside(near)
            odd = carry[0] + fold(now * near)
            even = carry[1] + fold(inside(new_w) * near)
            if first:
                return (odd, even, carry[2] + fold(now * now / inside(inverse)))
            return (odd, even)

        zero = jnp.zeros((8, cz), F32)
        sums = lax.fori_loop(0, cx // 8, one, (zero,) * (3 if first else 2), unroll=True)
        for r in (LOW - 4, LOW + cx):
            new[pl.ds(r, 4)] = de[pl.ds(r, 4)] * around_sum(ref, r, 4)
        return sums

    with jax.named_scope("step#k=0"):
        mu1, mu2, mu0 = step(w0, w1, True)
    with jax.named_scope("step#k=1"):
        mu3, mu4 = step(w1, w2, False)

    def final(i, carry):
        near = inside(around_sum(w2, LOW + 8 * i, 8))
        last[pl.ds(8 * i, 8)] = near
        return carry + fold(inside(w2[pl.ds(LOW + 8 * i, 8)]) * near)

    with jax.named_scope("step#k=2"):
        mu5 = lax.fori_loop(0, cx // 8, final, jnp.zeros((8, cz), F32), unroll=True)
    lines = [jnp.sum(v, axis=0, keepdims=True) for v in (mu0, mu1, mu2, mu3, mu4, mu5)]
    lines.append(jnp.zeros((2, cz), F32))
    sums = jnp.sum(jnp.concatenate(lines, axis=0), axis=1, keepdims=True)
    local = jnp.sum(jnp.where(iota((8, 128), 0) == iota((8, 128), 1), sums, 0.0), axis=0, keepdims=True)
    sends = []

    def reduce(stage, value, slots, me, peers):
        sum_out[stage] = value
        slots[me] = value
        for at in peers:
            remote(sum_out.at[stage], slots.at[me], ar_send.at[stage], ar_recv.at[stage], at).start()
        every = slots.at[pl.ds(0, len(peers))]
        everyone = remote(every, every, ar_send.at[stage], ar_recv.at[stage], peers[0])
        everyone.wait_recv()
        sends.append(everyone)
        return jnp.sum(slots[...], axis=0)

    others = [(d, e) for d in range(nx) for e in range(ny) if (d, e) != (0, 0)]
    others.sort(key=lambda o: -min(o[0], nx - o[0]) - min(o[1], ny - o[1]))
    far_first = sorted(range(1, ns), key=lambda n: -min(n, ns - n))
    with jax.named_scope("reduce#k=0"):
        local = reduce(0, local, sum_plane, f, [on_plane(d, e) for d, e in others])
    with jax.named_scope("reduce#k=1"):
        local = reduce(1, local, sum_line, s, [on_line(n) for n in far_first])
    lane = iota((1, 128), 1)
    mu = [jnp.sum(jnp.where(lane == k, local, 0.0), axis=1, keepdims=True) for k in range(6)]
    mu = [jnp.broadcast_to(m, (1, 128)) for m in mu]

    def product(u, v):
        out = 0.0
        for a, left in enumerate(u):
            for b, right in enumerate(v):
                out = out + left * right * mu[a + b]
        return out

    one_line = jnp.ones((1, cz), F32)
    course, misfit, guess = [one_line], [one_line], []
    rz = mu[0]
    for it in range(ITERS):
        image = [
            (course[k] if k < len(course) else 0.0) - (course[k - 1] if k > 0 else 0.0)
            for k in range(len(course) + 1)
        ]
        alpha = rz / product(course, image)
        guess = [(guess[k] if k < len(guess) else 0.0) + alpha * course[k] for k in range(len(course))]
        misfit = [(misfit[k] if k < len(misfit) else 0.0) - alpha * image[k] for k in range(len(image))]
        if it + 1 < ITERS:
            new = product(misfit, misfit)
            ratio = new / rz
            course = [misfit[k] + (ratio * course[k] if k < len(course) else 0.0) for k in range(len(misfit))]
            rz = new

    coefs[...] = jnp.concatenate(guess + misfit + [one_line], axis=0)
    with jax.named_scope("sent"):
        for copy in [spread_all, coded, jacs, ring_all, rows_all, cross_all] + sends:
            copy.wait_send()


def finish(field, w0, w1, w2, last, coefs, guess, misfit):
    xe, de = field.at[0], field.at[1]
    n, cy, _ = guess.shape
    first = pl.program_id(0) * n
    here = (pl.ds(LOW + first, n), pl.ds(SIDE, cy))
    line = [coefs[k : k + 1, :] for k in range(7)]
    basis = [w0[here], w1[here], w2[here]]
    guess[...] = xe[here] + (line[0] * basis[0] + (line[1] * basis[1] + line[2] * basis[2]))
    rest = line[3] * basis[0] + (line[4] * basis[1] + line[5] * basis[2])
    misfit[...] = rest / de[here] + line[6] * last[pl.ds(first, n)]


def per_device(nx, ny, nz, x0, c, b, j, owner, slot):
    quads, faces = b.shape
    rows = slot.shape[0]
    cx, cy, cz = x0.shape
    share = quads // nx
    deep = faces * share // 128
    half = ny // 2
    wide = (cx + 10, cy + 16, cz)
    lines = rows // 128
    nf, ns = nx * ny, nz * CORES
    dma = pltpu.SemaphoreType.DMA
    vmem = pltpu.VMEM
    scratch = [
        vmem((quads, faces), F32), vmem((quads, rows), F32), vmem((2, lines, 128), jnp.int32),
        vmem((nx, deep, 128), F32), vmem((ny, nx, deep, 128), F32), vmem((nx, share, rows), F32),
        vmem((nx, lines, 128), jnp.int32), vmem((lines, 128), jnp.int32),
        vmem((nx * rows, 128), F32), vmem((nx * rows, 128), F32), vmem((nx * rows, 128), F32),
        vmem((nx * lines + 2, 1, 128), F32), vmem((3 * nx, lines + 2, 1, 128), F32), vmem((2, 3 * nx, 1, 128), F32), vmem((8, 128), F32),
        vmem((2, 1, 128), F32), vmem((nf, 1, 128), F32), vmem((ns, 1, 128), F32),
        dma((6,)), dma, dma((nx - 1,)), dma, dma, dma, dma,
        dma, dma((2, half, nx)), dma((4,)), dma((4,)), dma, dma, dma, dma((2,)), dma((2,)), dma((2,)),
        pltpu.SemaphoreType.REGULAR((4, 2)), vmem((2 * nx * deep, 256), BF16),
    ]
    wide_out = jax.ShapeDtypeStruct(wide, F32)
    out = jax.ShapeDtypeStruct((cx, cy, cz), F32)
    whole = pl.BlockSpec(memory_space=vmem)
    operands = (x0, c, b, j, owner.reshape(lines, 128), slot.reshape(lines, 128))
    state = pl.pallas_call(
        functools.partial(body, nx, ny, nz),
        out_shape=(jax.ShapeDtypeStruct((2,) + wide, F32),) + (wide_out,) * 3 + (out, jax.ShapeDtypeStruct((8, 128), F32)),
        in_specs=[pl.BlockSpec(memory_space=pltpu.HBM)] * 6,
        out_specs=(whole,) * 6,
        scratch_shapes=scratch,
        compiler_params=pltpu.CompilerParams(collective_id=0, has_side_effects=True, vmem_limit_bytes=44 * 2**20),
        name="coupling_step",
    )(*[pltpu.with_memory_space_constraint(v, pltpu.HBM) for v in operands])
    chunk = pl.BlockSpec((cx // 2, cy, cz), lambda i: (i, 0, 0))
    return pl.pallas_call(
        finish,
        grid=(2,),
        out_shape=(out, out),
        in_specs=[whole] * 6,
        out_specs=(chunk, chunk),
        compiler_params=pltpu.CompilerParams(vmem_limit_bytes=16 * 2**20),
        name="finish_step",
    )(*state)


def solution(mesh):
    nx, nz = XCHIPS, mesh.shape["solid"] // CORES
    ny = mesh.shape["fluid"] // nx
    both = ("fluid", "solid")
    block = P("fluid", "solid", None)
    return jax.shard_map(
        functools.partial(per_device, nx, ny, nz),
        mesh=mesh,
        in_specs=(block, block, P(None, both), P(None, both), P(both, None), P(both)),
        out_specs=(block, block),
        check_vma=False,
    )
```

```python
import functools

import jax
import jax.numpy as jnp
from jax import lax
from jax.experimental import pallas as pl
from jax.experimental.pallas import tpu as pltpu
from jax.sharding import PartitionSpec as P

ITERS = 3
XCHIPS = 4
CORES = 2
MESH = pl.DeviceIdType.MESH
F32 = jnp.float32
BF16 = jnp.bfloat16
AROUND = [(a, b) for a in (-1, 0, 1) for b in (-1, 0, 1) if (a, b) != (0, 0)]
LOW = 5
SIDE = 8


def iota(shape, axis):
    return lax.broadcasted_iota(jnp.int32, shape, axis)


def body(
    nx, ny, nz,
    x0_hbm, c_hbm, b_hbm, j_hbm, owner_hbm, slot_hbm,
    field, w0, w1, w2, last, coefs,
    bv, jv, idx, tabs, held, jac, codes, code_own, key, jm, acc,
    part_out, part_in, cross_in, edge, sum_out, sum_plane, sum_line,
    load_sem, bx_send, bx_recv, jx_send, jx_recv, cx_send, cx_recv,
    ring_send, ring_recv, halo_send, halo_recv, row_send, row_recv, cross_send, cross_recv, ar_send, ar_recv, tokens, tables,
):
    xe, de = field.at[0], field.at[1]
    cx, cy, cz = (xe.shape[0] - 10, xe.shape[1] - 16, xe.shape[2])
    quads, faces = bv.shape
    rows = jv.shape[1]
    share = quads // nx
    many = 128 // share
    deep = faces // many
    rowsets = rows // 128
    f, s = lax.axis_index("fluid"), lax.axis_index("solid")
    nf, ns = nx * ny, nz * CORES
    x, y = lax.rem(f, nx), f // nx

    def remote(src, dst, send, recv, at):
        return pltpu.make_async_remote_copy(
            src_ref=src, dst_ref=dst, send_sem=send, recv_sem=recv,
            device_id=at, device_id_type=MESH,
        )

    def beside(a, b):
        return (lax.rem(f + a + nf, nf), lax.rem(s + b + ns, ns))

    def on_x(d):
        return (y * nx + lax.rem(x + d, nx), s)

    def on_y(d):
        return (lax.rem(y + d, ny) * nx + x, s)

    def in_row(a, d, b):
        return (lax.rem(y + a + ny, ny) * nx + lax.rem(x + d, nx), lax.rem(s + b + ns, ns))

    def on_plane(d, e):
        return (lax.rem(y + e, ny) * nx + lax.rem(x + d, nx), s)

    def on_line(n):
        return (f, lax.rem(s + n, ns))

    inner = (pl.ds(LOW, cx), pl.ds(SIDE, cy))
    loads = [
        pltpu.make_async_copy(b_hbm, bv, load_sem.at[0]),
        pltpu.make_async_copy(owner_hbm, idx.at[0], load_sem.at[1]),
        pltpu.make_async_copy(slot_hbm, idx.at[1], load_sem.at[2]),
        pltpu.make_async_copy(j_hbm, jv, load_sem.at[3]),
        pltpu.make_async_copy(x0_hbm, xe.at[inner], load_sem.at[4]),
        pltpu.make_async_copy(c_hbm, de.at[inner], load_sem.at[5]),
    ]
    for load in loads:
        load.start()

    barrier = pltpu.get_barrier_semaphore()
    partners = [on_x(d) for d in range(1, nx)] + [on_y(1), on_y(ny - 1), beside(0, -1), beside(0, 1)]
    for at in partners:
        pl.semaphore_signal(barrier, inc=1, device_id=at, device_id_type=MESH)

    def tell(kind, low, high):
        pl.semaphore_signal(tokens.at[kind, 0], inc=1, device_id=low, device_id_type=MESH)
        pl.semaphore_signal(tokens.at[kind, 1], inc=1, device_id=high, device_id_type=MESH)

    def hear(kind):
        pl.semaphore_wait(tokens.at[kind, 0], 1)
        pl.semaphore_wait(tokens.at[kind, 1], 1)

    guard = jnp.zeros(xe.shape[1:], F32)
    for ref in (xe, w0, w1, w2):
        ref[0] = guard
        ref[cx + 9] = guard

    for end in (0, nx * rowsets + 1):
        part_out[end] = jnp.zeros((1, 128), F32)

    with jax.named_scope("tables"):
        loads[0].wait()
        for a in range(nx):
            mine = bv[a * share : (a + 1) * share, :]
            stack = jnp.concatenate(
                [mine[:, (m * deep // 128) * 128 : (m * deep // 128) * 128 + 128] for m in range(many)], axis=0
            )
            if deep < 128:
                turned = pltpu.roll(stack, 128 - deep, 1)
                odd = (iota(stack.shape, 0) // share) % 2 == 1
                stack = jnp.where(odd, turned, stack)
            tabs[a] = stack.T[:deep]
        loads[1].wait()
        loads[2].wait()
        code_own[...] = idx[0] * faces + idx[1]
        codes[0] = code_own[...]
        held[y, 0] = tabs[x]

    with jax.named_scope("entry"):
        pl.semaphore_wait(barrier, len(partners))
        tell(0, beside(0, -1), beside(0, 1))

    def ring(t, d, way):
        slot = lax.rem(y + ny + (1 - t if way == 0 else t - 1), ny)
        at = on_y(1 if way == 0 else ny - 1)
        block = held.at[slot, d]
        return remote(block, block, ring_send, ring_recv.at[way, t - 1, d], at)

    half = ny // 2

    def goes(t, d, way):
        return t < half or (d < nx // 2) == (way == 0)

    ways = [
        [[ring(t, d, way) if goes(t, d, way) else None for way in range(2)] for d in range(nx)]
        for t in range(1, half + 1)
    ]

    def forward(t, d):
        if t == 1 and d > 0:
            spread[d - 1].wait_recv()
        for way in range(2):
            if t > 1:
                ways[t - 2][d][way].wait_recv()
            if goes(t, d, way):
                ways[t - 1][d][way].start()

    forward(1, 0)
    spread = []
    for d in range(1, nx):
        remote(code_own, codes.at[d], cx_send, cx_recv, on_x(d)).start()
    some = pl.ds(0, nx - 1)
    coded = remote(codes.at[some], codes.at[some], cx_send, cx_recv, on_x(1))
    jacs = remote(jac.at[some], jac.at[some], jx_send, jx_recv, on_x(1))
    spread_all = remote(tabs.at[some], tabs.at[some], bx_send, bx_recv.at[0], on_x(1))
    ring_all = remote(held.at[pl.ds(0, ny - 1)], held.at[pl.ds(0, ny - 1)], ring_send, bx_recv.at[0], on_x(1))
    for d in range(1, nx):
        to = lax.rem(x + d, nx)
        spread.append(remote(tabs.at[to], held.at[y, d], bx_send, bx_recv.at[d - 1], on_x(d)))
        spread[-1].start()

    def prepare_keys(d):
        for i in range(rowsets):
            code = codes[d, i : i + 1, :]
            owner, slot = code // faces, lax.rem(code, faces)
            keys = (owner * deep + lax.rem(slot, deep)).astype(F32)
            key[d * rows + i * 128 : d * rows + (i + 1) * 128, :] = jnp.broadcast_to(keys, (128, 128)).T

    def prepare_jac(d):
        for i in range(rowsets):
            slot = lax.rem(codes[d, i : i + 1, :], faces)
            j = jac[d, :, i * 128 : (i + 1) * 128]
            tiled = jnp.concatenate([j] * many, axis=0)
            wanted = iota((128, 128), 0) // share == jnp.broadcast_to(slot // deep, (128, 128))
            jm[d * rows + i * 128 : d * rows + (i + 1) * 128, :] = jnp.where(wanted, tiled, 0.0).T

    def weight(slot):
        parts = []
        for d in range(nx):
            parts.append(held[slot, d])
        table = jnp.concatenate(parts, axis=0)
        high = table.astype(BF16)
        low = (table - high.astype(F32)).astype(BF16)
        return jnp.concatenate([high, low], axis=1)

    def base_of(slot, d):
        return (slot * nx + lax.rem(x - d + nx, nx)) * deep

    tall = rows

    def pick(d, slots, fresh, first=False, finish=None):
        if fresh:
            for n, slot in enumerate(slots):
                tables[n * nx * deep : (n + 1) * nx * deep, :] = weight(slot)
        table = tables[: len(slots) * nx * deep, :]
        lanes = iota((1, 128), 1)
        marks = []
        for slot in slots:
            for tile in range(nx * deep // 128):
                mark = jnp.zeros((1, 128), jnp.int32)
                for e in range(128 // deep):
                    p = tile * (128 // deep) + e
                    mark = jnp.where(lanes // deep == e, base_of(slot, p) + lanes - e * deep, mark)
                marks.append(mark.astype(F32))
        for i in range(rows // tall):
            start = d * rows + i * tall
            place = pl.ds(start if isinstance(start, int) else pl.multiple_of(start, tall), tall)
            keys = key[place, :]
            hot = jnp.concatenate([jnp.where(keys == mark, 1.0, 0.0).astype(BF16) for mark in marks], axis=1)
            both = jnp.dot(hot, table, preferred_element_type=F32)
            got = both[:, :128] + both[:, 128:]
            if not first:
                got = got + acc[place, :]
            if finish is None:
                acc[place, :] = got
                continue
            product = got * jm[place, :]
            for k in range(tall // 128):
                line = jnp.sum(product[k * 128 : (k + 1) * 128].T, axis=0, keepdims=True)
                at = i * (tall // 128) + k
                part_out[1 + finish * rowsets + at] = line

    def around_sum(ref, r, n):
        mid = ref[pl.ds(r, n)].reshape(n * xe.shape[1], cz)
        out = ref[pl.ds(r - 1, n)] + ref[pl.ds(r + 1, n)]
        out = out.reshape(n * xe.shape[1], cz)
        out = out + (pltpu.roll(mid, 1, 0) + pltpu.roll(mid, mid.shape[0] - 1, 0))
        lane = iota(mid.shape, 1)
        out = out + jnp.where(lane == 0, 0.0, pltpu.roll(mid, 1, 1))
        out = out + jnp.where(lane == cz - 1, 0.0, pltpu.roll(mid, cz - 1, 1))
        return out.reshape(n, xe.shape[1], cz)

    def start_solid():
        for ref, fill in ((xe, 0.0), (de, 1e30)):
            @pl.when(f == 0)
            def _():
                ref[pl.ds(LOW - 4, 4)] = jnp.full((4,) + xe.shape[1:], fill, F32)

            @pl.when(f == nf - 1)
            def _():
                ref[pl.ds(LOW + cx, 4)] = jnp.full((4,) + xe.shape[1:], fill, F32)

            @pl.when(s == 0)
            def _():
                ref[pl.ds(1, cx + 8), pl.ds(0, 8)] = jnp.full((cx + 8, 8, cz), fill, F32)

            @pl.when(s == ns - 1)
            def _():
                ref[pl.ds(1, cx + 8), pl.ds(SIDE + cy, 8)] = jnp.full((cx + 8, 8, cz), fill, F32)

        def one(i, carry):
            r = 1 + 8 * i
            got = around_sum(xe, r, 8) - 6.0 * xe[pl.ds(r, 8)]
            c = de[pl.ds(r, 8)]
            inverse = jnp.where(c > 1e29, 0.0, 1.0 / (6.0 + c))
            de[pl.ds(r, 8)] = inverse
            w0[pl.ds(r, 8)] = inverse * got
            return carry

        lax.fori_loop(0, (cx + 8) // 8, one, 0)

    order = sorted(range(nx), key=lambda d: (min(d, nx - d), -d))

    def round_of(t):
        others = [(t, d) for d in order if d > 0]
        ahead = [(t + 2, 0)] if t + 2 <= half else []
        return ([(2, 0)] if t == 1 and half > 1 else []) + others + ahead

    prepare_keys(0)
    for n, (t, d) in enumerate(round_of(1)):
        with jax.named_scope(f"forward#t={t}#d={d}"):
            forward(t, d)
        if (t, d) == (1, order[1]):
            coded.wait_recv()
        if t == 1:
            prepare_keys(d)
    with jax.named_scope("hear#k=0"):
        hear(0)
        for load in loads[3:]:
            load.wait()
        jac[0] = jv[pl.ds(pl.multiple_of(x * share, share), share), :]
    tell(1, on_y(ny - 1), on_y(1))
    if ns > 4:
        tell(2, beside(0, -2), beside(0, 2))
    for d in range(1, nx):
        to = lax.rem(x + d, nx)
        remote(
            jv.at[pl.ds(pl.multiple_of(to * share, share), share)], jac.at[d], jx_send, jx_recv, on_x(d)
        ).start()
    to_y = {-1: (pl.ds(SIDE, 8), pl.ds(SIDE + cy, 8)), 0: (pl.ds(SIDE, cy),) * 2, 1: (pl.ds(SIDE + cy - 8, 8), pl.ds(SIDE - 8, 8))}

    def send_side(a):
        def rows_of(count):
            if a == 1:
                return pl.ds(LOW + cx - count, count), pl.ds(LOW - count, count)
            return pl.ds(LOW, count), pl.ds(LOW + cx, count)

        near, near_to = rows_of(3)
        four, four_to = rows_of(4)
        fourth = pl.ds(LOW + cx - 4 if a == 1 else LOW + 3, 1)
        fourth_to = pl.ds(LOW - 4 if a == 1 else LOW + cx + 3, 1)
        sides = pl.ds(SIDE, cy)
        cuts = [
            (field.at[:, near, sides], field.at[:, near_to, sides], 1, 0),
            (field.at[0, fourth, sides], field.at[0, fourth_to, sides], 2, 0),
            (field.at[:, near, pl.ds(SIDE + cy - 4, 4)], field.at[:, near_to, pl.ds(SIDE - 4, 4)], 3, 1),
            (field.at[:, near, pl.ds(SIDE, 4)], field.at[:, near_to, pl.ds(SIDE + cy, 4)], 3, -1),
        ]
        for src, dst, k, b in cuts:
            remote(src, dst, halo_send.at[k], halo_recv.at[k], beside(a, b)).start()

    ends = ((1, nx - 1), (-1, 0))

    def send_sides(inside):
        for a, end in ends:
            @pl.when((x != end) if inside else (x == end))
            def _():
                send_side(a)

    for b in (-1, 1):
        remote(
            field.at[:, pl.ds(LOW, cx), to_y[b][0]], field.at[:, pl.ds(LOW, cx), to_y[b][1]],
            halo_send.at[0], halo_recv.at[0], beside(0, b),
        ).start()
    send_sides(True)
    rims = [
        field.at[:, pl.ds(LOW, cx), pl.ds(0, 16)],
        field.at[:, pl.ds(LOW - 3, 6), pl.ds(SIDE, cy)],
        field.at[0, pl.ds(LOW - 4, 2), pl.ds(SIDE, cy)],
        field.at[:, pl.ds(LOW - 3, 6), pl.ds(0, 8)],
    ]
    halos = [remote(rim, rim, halo_send.at[k], halo_recv.at[k], on_x(1)) for k, rim in enumerate(rims)]

    def near(far):
        if far == 0:
            return [y]
        return [lax.rem(y + ny - far, ny), lax.rem(y + far, ny)]

    unprepared = list(order)

    def next_jac():
        with jax.named_scope(f"prepare_jac#n={len(unprepared)}"):
            if len(unprepared) == nx:
                jacs.wait_recv()
            prepare_jac(unprepared.pop(0))

    def hear_more():
        hear(1)
        if ns > 4:
            hear(2)
        if ns > 8:
            tell(3, beside(0, -4), beside(0, 4))

    for t in range(2, half + 1):
        todo = round_of(t)
        for n, d in enumerate(order):
            if n < len(todo):
                with jax.named_scope(f"forward#t={t}#n={n}"):
                    forward(*todo[n])
            with jax.named_scope(f"pick#t={t}#d={d}"):
                pick(d, near(t - 2), n == 0, first=t == 2)
            if t == max(2, half - 1) and n == 0:
                hear_more()
            if (t == half - 1 and n % 2 == 1) or (t == half and n < 2):
                next_jac()
    send_sides(False)
    if half == 1:
        hear_more()
    while unprepared:
        next_jac()
    for d in range(nx):
        with jax.named_scope(f"pick_near#d={d}"):
            pick(d, near(half - 1), d == 0, first=half == 1)
    if ns > 8:
        with jax.named_scope("hear#k=3"):
            hear(3)
    with jax.named_scope("far_wait"):
        for d in range(nx):
            for way in range(2):
                if goes(half, d, way):
                    ways[half - 1][d][way].wait_recv()
    def share_ends(b):
        slot = (1 - b) * nx + x
        line = part_out.at[nx * rowsets]
        remote(line, cross_in.at[0, slot], cross_send, cross_recv.at[0], in_row(1, nx - x, b)).start()
        line = part_out.at[1]
        remote(line, cross_in.at[1, slot], cross_send, cross_recv.at[1], in_row(-1, 2 * nx - 1 - x, b)).start()

    def share_rows(b):
        slot = (1 - b) * nx + x
        for d in order[::-1]:
            if (d, b) != (0, 0):
                lines = part_out.at[pl.ds(lax.rem(x + d, nx) * rowsets, rowsets + 2)]
                remote(lines, part_in.at[slot], row_send, row_recv, in_row(0, d, b)).start()

    readers = [0, nx - 1] + list(range(1, nx - 1))
    for n, reader in enumerate(readers):
        with jax.named_scope(f"pick_far#d={reader}"):
            pick(lax.rem(x - reader + nx, nx), [lax.rem(y + half, ny)], n == 0, finish=reader)
        if n == 2:
            for b in (1, -1, 0):
                share_ends(b)
    for b in (1, -1, 0):
        share_rows(b)
    part_in[nx + x] = part_out[pl.ds(x * rowsets, rowsets + 2)]
    most = part_in.at[pl.ds(0, 3 * nx - 1)]
    rows_all = remote(most, most, row_send, row_recv, on_x(1))
    six = cross_in.at[0, pl.ds(0, 6)]
    cross_all = remote(six, six, cross_send, cross_recv.at[0], on_x(1))
    with jax.named_scope("solid_wait"):
        for halo in halos:
            halo.wait_send()
        for halo in halos:
            halo.wait_recv()
    with jax.named_scope("solid_start"):
        start_solid()
    with jax.named_scope("part_wait"):
        rows_all.wait_recv()
        for side, end in ((0, 0), (1, nx - 1)):
            @pl.when(x == end)
            def _():
                whole = cross_in.at[side]
                remote(whole, whole, cross_send, cross_recv.at[side], on_x(1)).wait_recv()

    per = 128 // cy

    def heat(r, first, count, line, offset):
        shape = (per, count, 128)
        spot = iota(shape, 2)
        picked = jnp.where(spot == iota(shape, 0) * cy + iota(shape, 1) + offset, line.reshape(1, 1, 128), 0.0)
        column = jnp.sum(picked, axis=2, keepdims=True)
        here = (pl.ds(r, per), pl.ds(first, count))
        w0[here] = w0[here] + jnp.where(spot == cz - 1, column * de[here], 0.0)

    def gathered(b, spot):
        return sum(part_in[(b + 1) * nx + h, spot] for h in range(nx))

    with jax.named_scope("heat"):
        for a, end, side, spot in ((1, nx - 1, 1, rowsets + 1), (-1, 0, 0, 0)):
            for b in (-1, 0, 1):
                here = pl.ds(3 * side + b + 1, 1)

                @pl.when(x == end)
                def _():
                    edge[here, :] = sum(cross_in[side, (b + 1) * nx + h] for h in range(nx))

                @pl.when(x != end)
                def _():
                    edge[here, :] = gathered(b, spot)

        for a in (-1, 0, 1):
            for b in (-1, 0, 1):
                first = {0: SIDE, -1: 0, 1: SIDE + cy}[b]
                count = {0: cy, -1: 8, 1: 8}[b]
                offset = {0: 0, -1: cy - 8, 1: 0}[b]
                if a == 0:
                    for i in range(cx // per):
                        heat(LOW + i * per, first, count, gathered(b, 1 + i), offset)
                else:
                    at = 3 * (1 if a == 1 else 0) + b + 1
                    heat(LOW + cx if a == 1 else LOW - 4, first, count, edge[at : at + 1, :], offset)

    def fold(v):
        return jnp.sum(v.reshape(-1, 8, cz), axis=0)

    def inside(v):
        return v[:, SIDE : SIDE + cy]

    def step(ref, new, first):
        def one(i, carry):
            r = LOW + 8 * i
            near = around_sum(ref, r, 8)
            inverse = de[pl.ds(r, 8)]
            new_w = inverse * near
            new[pl.ds(r, 8)] = new_w
            now = inside(ref[pl.ds(r, 8)])
            near = inside(near)
            odd = carry[0] + fold(now * near)
            even = carry[1] + fold(inside(new_w) * near)
            if first:
                return (odd, even, carry[2] + fold(now * now / inside(inverse)))
            return (odd, even)

        zero = jnp.zeros((8, cz), F32)
        sums = lax.fori_loop(0, cx // 8, one, (zero,) * (3 if first else 2), unroll=True)
        for r in (LOW - 4, LOW + cx):
            new[pl.ds(r, 4)] = de[pl.ds(r, 4)] * around_sum(ref, r, 4)
        return sums

    with jax.named_scope("step#k=0"):
        mu1, mu2, mu0 = step(w0, w1, True)
    with jax.named_scope("step#k=1"):
        mu3, mu4 = step(w1, w2, False)

    def final(i, carry):
        near = inside(around_sum(w2, LOW + 8 * i, 8))
        last[pl.ds(8 * i, 8)] = near
        return carry + fold(inside(w2[pl.ds(LOW + 8 * i, 8)]) * near)

    with jax.named_scope("step#k=2"):
        mu5 = lax.fori_loop(0, cx // 8, final, jnp.zeros((8, cz), F32), unroll=True)
    lines = [jnp.sum(v, axis=0, keepdims=True) for v in (mu0, mu1, mu2, mu3, mu4, mu5)]
    lines.append(jnp.zeros((2, cz), F32))
    sums = jnp.sum(jnp.concatenate(lines, axis=0), axis=1, keepdims=True)
    local = jnp.sum(jnp.where(iota((8, 128), 0) == iota((8, 128), 1), sums, 0.0), axis=0, keepdims=True)
    sends = []

    def reduce(stage, value, slots, me, peers):
        sum_out[stage] = value
        slots[me] = value
        for at in peers:
            remote(sum_out.at[stage], slots.at[me], ar_send.at[stage], ar_recv.at[stage], at).start()
        every = slots.at[pl.ds(0, len(peers))]
        everyone = remote(every, every, ar_send.at[stage], ar_recv.at[stage], peers[0])
        everyone.wait_recv()
        sends.append(everyone)
        return jnp.sum(slots[...], axis=0)

    others = [(d, e) for d in range(nx) for e in range(ny) if (d, e) != (0, 0)]
    others.sort(key=lambda o: -min(o[0], nx - o[0]) - min(o[1], ny - o[1]))
    far_first = sorted(range(1, ns), key=lambda n: -min(n, ns - n))
    with jax.named_scope("reduce#k=0"):
        local = reduce(0, local, sum_plane, f, [on_plane(d, e) for d, e in others])
    with jax.named_scope("reduce#k=1"):
        local = reduce(1, local, sum_line, s, [on_line(n) for n in far_first])
    lane = iota((1, 128), 1)
    mu = [jnp.sum(jnp.where(lane == k, local, 0.0), axis=1, keepdims=True) for k in range(6)]
    mu = [jnp.broadcast_to(m, (1, 128)) for m in mu]

    def product(u, v):
        out = 0.0
        for a, left in enumerate(u):
            for b, right in enumerate(v):
                out = out + left * right * mu[a + b]
        return out

    one_line = jnp.ones((1, cz), F32)
    course, misfit, guess = [one_line], [one_line], []
    rz = mu[0]
    for it in range(ITERS):
        image = [
            (course[k] if k < len(course) else 0.0) - (course[k - 1] if k > 0 else 0.0)
            for k in range(len(course) + 1)
        ]
        alpha = rz / product(course, image)
        guess = [(guess[k] if k < len(guess) else 0.0) + alpha * course[k] for k in range(len(course))]
        misfit = [(misfit[k] if k < len(misfit) else 0.0) - alpha * image[k] for k in range(len(image))]
        if it + 1 < ITERS:
            new = product(misfit, misfit)
            ratio = new / rz
            course = [misfit[k] + (ratio * course[k] if k < len(course) else 0.0) for k in range(len(misfit))]
            rz = new

    coefs[...] = jnp.concatenate(guess + misfit + [one_line], axis=0)
    with jax.named_scope("sent"):
        for copy in [spread_all, coded, jacs, ring_all, rows_all, cross_all] + sends:
            copy.wait_send()


def finish(field, w0, w1, w2, last, coefs, guess, misfit):
    xe, de = field.at[0], field.at[1]
    n, cy, _ = guess.shape
    first = pl.program_id(0) * n
    here = (pl.ds(LOW + first, n), pl.ds(SIDE, cy))
    line = [coefs[k : k + 1, :] for k in range(7)]
    basis = [w0[here], w1[here], w2[here]]
    guess[...] = xe[here] + (line[0] * basis[0] + (line[1] * basis[1] + line[2] * basis[2]))
    rest = line[3] * basis[0] + (line[4] * basis[1] + line[5] * basis[2])
    misfit[...] = rest / de[here] + line[6] * last[pl.ds(first, n)]


def per_device(nx, ny, nz, x0, c, b, j, owner, slot):
    quads, faces = b.shape
    rows = slot.shape[0]
    cx, cy, cz = x0.shape
    share = quads // nx
    deep = faces * share // 128
    half = ny // 2
    wide = (cx + 10, cy + 16, cz)
    lines = rows // 128
    nf, ns = nx * ny, nz * CORES
    dma = pltpu.SemaphoreType.DMA
    vmem = pltpu.VMEM
    scratch = [
        vmem((quads, faces), F32), vmem((quads, rows), F32), vmem((2, lines, 128), jnp.int32),
        vmem((nx, deep, 128), F32), vmem((ny, nx, deep, 128), F32), vmem((nx, share, rows), F32),
        vmem((nx, lines, 128), jnp.int32), vmem((lines, 128), jnp.int32),
        vmem((nx * rows, 128), F32), vmem((nx * rows, 128), F32), vmem((nx * rows, 128), F32),
        vmem((nx * lines + 2, 1, 128), F32), vmem((3 * nx, lines + 2, 1, 128), F32), vmem((2, 3 * nx, 1, 128), F32), vmem((8, 128), F32),
        vmem((2, 1, 128), F32), vmem((nf, 1, 128), F32), vmem((ns, 1, 128), F32),
        dma((6,)), dma, dma((nx - 1,)), dma, dma, dma, dma,
        dma, dma((2, half, nx)), dma((4,)), dma((4,)), dma, dma, dma, dma((2,)), dma((2,)), dma((2,)),
        pltpu.SemaphoreType.REGULAR((4, 2)), vmem((2 * nx * deep, 256), BF16),
    ]
    wide_out = jax.ShapeDtypeStruct(wide, F32)
    out = jax.ShapeDtypeStruct((cx, cy, cz), F32)
    whole = pl.BlockSpec(memory_space=vmem)
    operands = (x0, c, b, j, owner.reshape(lines, 128), slot.reshape(lines, 128))
    state = pl.pallas_call(
        functools.partial(body, nx, ny, nz),
        out_shape=(jax.ShapeDtypeStruct((2,) + wide, F32),) + (wide_out,) * 3 + (out, jax.ShapeDtypeStruct((8, 128), F32)),
        in_specs=[pl.BlockSpec(memory_space=pltpu.HBM)] * 6,
        out_specs=(whole,) * 6,
        scratch_shapes=scratch,
        compiler_params=pltpu.CompilerParams(collective_id=0, has_side_effects=True, vmem_limit_bytes=44 * 2**20),
        name="coupling_step",
    )(*[pltpu.with_memory_space_constraint(v, pltpu.HBM) for v in operands])
    chunk = pl.BlockSpec((cx // 2, cy, cz), lambda i: (i, 0, 0))
    return pl.pallas_call(
        finish,
        grid=(2,),
        out_shape=(out, out),
        in_specs=[whole] * 6,
        out_specs=(chunk, chunk),
        compiler_params=pltpu.CompilerParams(vmem_limit_bytes=16 * 2**20),
        name="finish_step",
    )(*state)


def solution(mesh):
    nx, nz = XCHIPS, mesh.shape["solid"] // CORES
    ny = mesh.shape["fluid"] // nx
    both = ("fluid", "solid")
    block = P("fluid", "solid", None)
    return jax.shard_map(
        functools.partial(per_device, nx, ny, nz),
        mesh=mesh,
        in_specs=(block, block, P(None, both), P(None, both), P(both, None), P(both)),
        out_specs=(block, block),
        check_vma=False,
    )
```
